128 devices in a mesh: grp: 8 (over z, core), loc: 16 (over x, y).
Axes of the slice: x: 4, y: 4, z: 4, core: 2. Of those that a mesh axis runs over, the one named last changes fastest.
Arguments:
- tokens: bfloat16 [16384, 2048], P(('grp', 'loc')), may hold values from -6 to 6
- expert_ids: int32 [16384, 6], P(('grp', 'loc')), may hold values from 0 to 63, as said below
- gate_weights: bfloat16 [16384, 6], P(('grp', 'loc')), may hold values from 0.099609375 to 1
- w_gate: bfloat16 [128, 2048, 704], P(('grp', 'loc')), may hold values from -0.125 to 0.125
- w_up: bfloat16 [128, 2048, 704], P(('grp', 'loc')), may hold values from -0.125 to 0.125
- w_down: bfloat16 [128, 704, 2048], P(('grp', 'loc')), may hold values from -0.15625 to 0.15625
Outputs:
- moe_out: bfloat16 [16384, 2048], P(('grp', 'loc'))
The draws below stay inside these ranges and needn't reach their ends.
Inputs may be any that keep to these rules, and one draw needn't show every extreme that they name: `expert_ids`: each row names 6 different experts in increasing order; they lie in exactly 4 of the 8 groups, expert e belonging to group e // 8.
All inputs are finite; a program needn't handle non-finite values.
Results may differ from the reference program's by a relative error of at most 0.008.
Values may be sent and summed in bfloat16 or wider, within the bound.
No kernel may reach another device: no remote copies, remote signals or barrier semaphores. Data moves between devices by JAX's collectives and lax.ppermute only.
A program may use at most 128 MiB of HBM per device.

```python
import math
import jax
import jax.numpy as jnp
from jax import lax

D = 2048
FF = 1408
TOPK = 6
GROUP_LIMIT = 4
TOK_DEV = 128
TOKENS = 16384
EXPERTS = 64
CAP = 18
N_GRP = 8


def draw_expert_ids(key, part):
    group_size = EXPERTS // N_GRP
    key_pop = jax.random.fold_in(key, 11)
    key_grp = jax.random.fold_in(key, 12)
    key_exp = jax.random.fold_in(key, 13)
    popular = jax.random.randint(key_pop, (EXPERTS,), 0, 32768)
    group_score = jax.random.randint(key_grp, (TOKENS, N_GRP), 0, 65536) * N_GRP + jnp.arange(N_GRP, dtype=jnp.int32)[None, :]
    values_top, chosen = lax.top_k(group_score, GROUP_LIMIT)
    chosen_mask = jnp.any(chosen[:, :, None] == jnp.arange(N_GRP, dtype=jnp.int32)[None, None, :], axis=1)
    expert_score = (jax.random.randint(key_exp, (TOKENS, EXPERTS), 0, 65536) + popular[None, :]) * EXPERTS + jnp.arange(EXPERTS, dtype=jnp.int32)[None, :]
    allowed = jnp.repeat(chosen_mask, group_size, axis=1)
    masked = jnp.where(allowed, expert_score, -1)
    by_group = masked.reshape(TOKENS, N_GRP, group_size)
    best_each = jnp.argmax(by_group, axis=2).astype(jnp.int32) + jnp.arange(N_GRP, dtype=jnp.int32)[None, :] * group_size
    picked = jnp.take_along_axis(best_each, chosen, axis=1)
    taken = jnp.any(picked[:, :, None] == jnp.arange(EXPERTS, dtype=jnp.int32)[None, None, :], axis=1)
    remain_score = jnp.where(taken, -1, masked)
    values_more, extra_ids = lax.top_k(remain_score, TOPK - GROUP_LIMIT)
    return jnp.sort(jnp.concatenate([picked, extra_ids.astype(jnp.int32)], axis=1), axis=1).astype(jnp.int32)


def shard_levels(key, dims, shards, smallest, largest):
    loudness, own = 1.0, jax.random.fold_in(key, 6)
    for axis_at, blocks in shards:
        draws = jnp.exp(jax.random.uniform(jax.random.fold_in(own, axis_at), (blocks,), jnp.float32, smallest / len(shards), largest / len(shards)))
        loudness = loudness * jnp.repeat(draws, dims[axis_at] // blocks).reshape([-1 if axis == axis_at else 1 for axis in range(len(dims))])
    return loudness


def scatter_about(rng, dims, width, bound, shards=(), kind=jnp.bfloat16):
    loudness = shard_levels(rng, dims, shards, -0.22, 0.18) if shards else 1.0
    drawn = jax.random.normal(rng, dims, jnp.float32) * width * loudness
    return jnp.minimum(jnp.maximum(drawn, -bound), bound).astype(kind)


def setup_inputs(seed: int = 0) -> dict:
    arg_keys = jax.random.split(jax.random.key(seed), 7)
    tokens = scatter_about(arg_keys[0], (TOKENS, D), 1.0, 6.0, ((0, 128),))
    expert_ids = draw_expert_ids(jax.random.fold_in(arg_keys[6], 71), 0)
    gate_weights = jnp.clip(jnp.exp(math.log(1.0) - 2.306499 * jax.random.uniform(arg_keys[2], (TOKENS, TOPK), jnp.float32) ** shard_levels(arg_keys[2], (TOKENS, TOPK), ((0, 128),), -0.2, 0.2)), 0.099609375, 1.0).astype(jnp.bfloat16)
    w_gate = scatter_about(arg_keys[3], (2 * EXPERTS, D, FF // 2), D ** -0.5, 0.125, ((0, 128),))
    w_up = scatter_about(arg_keys[4], (2 * EXPERTS, D, FF // 2), D ** -0.5, 0.125, ((0, 128),))
    w_down = scatter_about(arg_keys[5], (2 * EXPERTS, FF // 2, D), FF ** -0.5, 0.15625, ((0, 128),))
    return {"tokens": tokens, "expert_ids": expert_ids, "gate_weights": gate_weights, "w_gate": w_gate, "w_up": w_up, "w_down": w_down}


def slot_block(block):
    onehot = (block[:, None] == jnp.arange(EXPERTS, dtype=jnp.int32)[None, :]).astype(jnp.int32)
    before = (jnp.cumsum(onehot, axis=0) - onehot).astype(jnp.int32)
    return jnp.sum(before * onehot, axis=1).astype(jnp.int32)


def reference(tokens, expert_ids, gate_weights, w_gate, w_up, w_down):
    devices = TOKENS // TOK_DEV
    per_group = EXPERTS // N_GRP
    rows_all = devices * CAP
    flat_ids = expert_ids.reshape(devices, TOK_DEV * TOPK)
    slot_of = lax.map(slot_block, flat_ids).reshape(TOKENS, TOPK).astype(jnp.int32)
    is_kept = slot_of < CAP
    token_index = jnp.arange(TOKENS, dtype=jnp.int32)
    row_base = (token_index // TOK_DEV) * CAP
    place_at = jnp.where(is_kept, row_base[:, None] + slot_of, rows_all).astype(jnp.int32)
    weights_kept = jnp.where(is_kept, gate_weights.astype(jnp.float32), jnp.float32(0.0))

    def expert_term(expert):
        matched = expert_ids == expert
        row_of = jnp.sum(jnp.where(matched, place_at, 0), axis=1) + jnp.where(jnp.any(matched, axis=1), 0, rows_all)
        row_of = row_of.astype(jnp.int32)
        weight = jnp.sum(jnp.where(matched, weights_kept, jnp.float32(0.0)), axis=1)
        buffer = jnp.zeros((rows_all + 1, D), jnp.bfloat16).at[row_of].set(tokens)
        summed = jnp.zeros((TOKENS, D), jnp.float32)
        for half_index in range(2):
            weight_row = 2 * expert + half_index
            gate_proj = jnp.dot(buffer, w_gate[weight_row], preferred_element_type=jnp.float32)
            up_proj = jnp.dot(buffer, w_up[weight_row], preferred_element_type=jnp.float32)
            hidden = (jax.nn.silu(gate_proj) * up_proj).astype(jnp.bfloat16)
            half_out = jnp.dot(hidden, w_down[weight_row], preferred_element_type=jnp.float32).astype(jnp.bfloat16)
            summed = summed + half_out[row_of].astype(jnp.float32)
        return weight[:, None] * summed

    def group_step(result, group_id):
        def add_expert(member, accumulated):
            expert = (group_id * per_group + member).astype(jnp.int32)
            return accumulated + expert_term(expert)

        accumulated = lax.fori_loop(0, per_group, add_expert, jnp.zeros((TOKENS, D), jnp.float32))
        rounded = lax.optimization_barrier(accumulated.astype(jnp.bfloat16))
        return result + rounded.astype(jnp.float32), None

    result, ignored = lax.scan(group_step, jnp.zeros((TOKENS, D), jnp.float32), jnp.arange(N_GRP, dtype=jnp.int32))
    return result.astype(jnp.bfloat16)
```

```python
import functools

import jax
import jax.numpy as jnp
from jax import lax
from jax.experimental import pallas as pl
from jax.experimental.pallas import tpu as pltpu
from jax.sharding import PartitionSpec as P

AXES = ("grp", "loc")
CAP = 18
MAIN = 16
PIECES = 8
TILE = MAIN * PIECES


def split_matrix():
    row = lax.broadcasted_iota(jnp.int32, (TILE, TILE), 0)
    col = lax.broadcasted_iota(jnp.int32, (TILE, TILE), 1)
    source = (row % MAIN) // 2 * MAIN + (row % 2) * PIECES + row // MAIN
    return (source == col).astype(jnp.bfloat16)


def exact_dot(a, b, dims=((1,), (0,))):
    return lax.dot_general(a, b, (dims, ((), ())), preferred_element_type=jnp.float32)


def pieces_to_rows(tile, matrix):
    stacked = exact_dot(matrix, tile).astype(jnp.bfloat16)
    return jnp.concatenate(
        [stacked[MAIN * q : MAIN * (q + 1)] for q in range(PIECES)], axis=1
    )


def rows_to_pieces(rows, matrix):
    width = rows.shape[1] // PIECES
    stacked = jnp.concatenate(
        [rows[:, width * q : width * (q + 1)] for q in range(PIECES)], axis=0
    )
    return exact_dot(matrix, stacked, ((0,), (0,))).astype(jnp.bfloat16)


def slots_of(ids_t, experts, gates_t=None):
    top, count = ids_t.shape
    expert = lax.broadcasted_iota(jnp.int32, (experts, count), 0)
    used = jnp.zeros((experts, count), jnp.float32)
    weight = jnp.zeros((experts, count), jnp.float32)
    for k in range(top):
        hit = expert == ids_t[k : k + 1, :]
        used = jnp.where(hit, 1.0, used)
        if gates_t is not None:
            weight = jnp.where(hit, gates_t[k : k + 1, :], weight)
    earlier = lax.broadcasted_iota(jnp.int32, (count, count), 0)
    later = lax.broadcasted_iota(jnp.int32, (count, count), 1)
    before = exact_dot(used.astype(jnp.bfloat16), (earlier < later).astype(jnp.bfloat16))
    return jnp.where(used > 0.0, before, -1.0), weight


def dispatch_kernel(ids_ref, tokens_ref, out_ref, slot_ref):
    block, _, _, width = out_ref.shape
    count, model = tokens_ref.shape
    step = pl.program_id(0)

    @pl.when(step == 0)
    def _():
        slot_ref[...] = slots_of(ids_ref[...], slot_ref.shape[0])[0]

    slot = slot_ref[pl.ds(pl.multiple_of(step * block, block), block), :]
    main_id = lax.broadcasted_iota(jnp.int32, (block, MAIN, count), 1).astype(jnp.float32)
    pick = (slot[:, None, :] == main_id).astype(jnp.float32).reshape(block * MAIN, count)
    rows = exact_dot(pick.astype(jnp.bfloat16), tokens_ref[...]).astype(jnp.bfloat16)
    rows = rows.reshape(block, MAIN, model)
    row = lax.broadcasted_iota(jnp.int32, (2 * block, count), 0)
    slot_twice = jnp.broadcast_to(slot[:, None, :], (block, 2, count)).reshape(2 * block, count)
    pick_last = (slot_twice == (MAIN + row % 2).astype(jnp.float32)).astype(jnp.bfloat16)
    last = exact_dot(pick_last, tokens_ref[...]).astype(jnp.bfloat16)
    pieces = rows_to_pieces(last, split_matrix()).reshape(block, MAIN, width - model)
    for half in range(2):
        out_ref[:, half, :, :model] = rows
        out_ref[:, half, :, model:] = pieces


def dispatch(ids_t, tokens, experts):
    count, model = tokens.shape
    width = model * CAP // MAIN
    block = 8
    return pl.pallas_call(
        dispatch_kernel,
        grid=(experts // block,),
        in_specs=[
            pl.BlockSpec(ids_t.shape, lambda i: (0, 0)),
            pl.BlockSpec(tokens.shape, lambda i: (0, 0)),
        ],
        out_specs=pl.BlockSpec((block, 2, MAIN, width), lambda i: (i, 0, 0, 0)),
        out_shape=jax.ShapeDtypeStruct((experts, 2, MAIN, width), jnp.bfloat16),
        scratch_shapes=[pltpu.VMEM((experts, count), jnp.float32)],
        cost_estimate=pl.CostEstimate(
            flops=4 * experts * CAP * count * model, bytes_accessed=4 * experts * MAIN * width,
            transcendentals=0,
        ),
        name="dispatch_rows",
    )(ids_t, tokens)


def ffn_kernel(x_ref, gate_ref, up_ref, down_ref, out_ref, rows_ref):
    block, _, width = x_ref.shape
    model = gate_ref.shape[1]
    main = block * MAIN
    matrix = split_matrix()
    rows_ref[:main, :] = x_ref[:, :, :model].reshape(main, model)
    pieces = x_ref[:, :, model:].reshape(main, width - model)
    for tile in range(main // TILE):
        rows_ref[main + MAIN * tile : main + MAIN * (tile + 1), :] = pieces_to_rows(
            pieces[TILE * tile : TILE * (tile + 1)], matrix
        )
    rows = rows_ref[...]
    gate = exact_dot(rows, gate_ref[0])
    up = exact_dot(rows, up_ref[0])
    hidden = (gate / (1.0 + jnp.exp(-gate)) * up).astype(jnp.bfloat16)
    half_out = exact_dot(hidden, down_ref[0]).astype(jnp.bfloat16)
    out_ref[:, :, :model] = half_out[:main].reshape(block, MAIN, model)
    for tile in range(main // TILE):
        piece = rows_to_pieces(half_out[main + MAIN * tile : main + MAIN * (tile + 1)], matrix)
        chunks = TILE // MAIN
        out_ref[chunks * tile : chunks * (tile + 1), :, model:] = piece.reshape(
            chunks, MAIN, width - model
        )


def half_ffn(chunks, w_gate, w_up, w_down):
    sources, _, width = chunks.shape
    model, hidden = w_gate.shape[1:]
    block = 32
    whole = lambda i: (0, 0, 0)
    return pl.pallas_call(
        ffn_kernel,
        grid=(sources // block,),
        in_specs=[
            pl.BlockSpec((block, MAIN, width), lambda i: (i, 0, 0)),
            pl.BlockSpec(w_gate.shape, whole, pipeline_mode=pl.Buffered(1)),
            pl.BlockSpec(w_up.shape, whole, pipeline_mode=pl.Buffered(1)),
            pl.BlockSpec(w_down.shape, whole, pipeline_mode=pl.Buffered(1)),
        ],
        out_specs=pl.BlockSpec((block, MAIN, width), lambda i: (i, 0, 0)),
        out_shape=jax.ShapeDtypeStruct(chunks.shape, jnp.bfloat16),
        scratch_shapes=[pltpu.VMEM((block * CAP, model), jnp.bfloat16)],
        cost_estimate=pl.CostEstimate(
            flops=6 * sources * CAP * model * hidden,
            bytes_accessed=4 * sources * CAP * model + 6 * model * hidden,
            transcendentals=sources * CAP * hidden,
        ),
        compiler_params=pltpu.CompilerParams(vmem_limit_bytes=56 * 1024 * 1024),
        name="half_ffn",
    )(chunks, w_gate, w_up, w_down)


def combine_kernel(ids_ref, gates_ref, rows_ref, out_ref, slot_ref, weight_ref, acc_ref):
    block, _, _, width = rows_ref.shape
    count, model = out_ref.shape
    step = pl.program_id(0)

    @pl.when(step == 0)
    def _():
        slot, weight = slots_of(ids_ref[...], slot_ref.shape[0], gates_ref[...])
        slot_ref[...] = slot
        weight_ref[...] = weight
        acc_ref[...] = jnp.zeros_like(acc_ref)

    here = pl.ds(pl.multiple_of(step * block, block), block)
    slot = slot_ref[here, :]
    weight = weight_ref[here, :]

    def spread(first, slots):
        shape = (block, 2 * slots, count)
        slot_id = first + lax.broadcasted_iota(jnp.int32, shape, 1) % slots
        hit = slot[:, None, :] == slot_id.astype(jnp.float32)
        scaled = jnp.where(hit, jnp.broadcast_to(weight[:, None, :], shape), 0.0)
        return scaled.reshape(block * 2 * slots, count).astype(jnp.bfloat16)

    rows = rows_ref[:, :, :, :model].reshape(block * 2 * MAIN, model)
    total = exact_dot(spread(0, MAIN), rows, ((0,), (0,)))
    matrix = split_matrix()
    pieces = rows_ref[:, :, :, model:].reshape(block * 2 * MAIN, width - model)
    last = jnp.concatenate(
        [
            pieces_to_rows(pieces[TILE * tile : TILE * (tile + 1)], matrix)
            for tile in range(block * 2 * MAIN // TILE)
        ],
        axis=0,
    )
    total += exact_dot(spread(MAIN, CAP - MAIN), last, ((0,), (0,)))
    acc_ref[...] += total

    @pl.when(step == pl.num_programs(0) - 1)
    def _():
        out_ref[...] = acc_ref[...].astype(jnp.bfloat16)


def combine(ids_t, gates_t, returned):
    experts, _, _, width = returned.shape
    count = ids_t.shape[1]
    model = width * MAIN // CAP
    block = 8
    return pl.pallas_call(
        combine_kernel,
        grid=(experts // block,),
        in_specs=[
            pl.BlockSpec(ids_t.shape, lambda i: (0, 0)),
            pl.BlockSpec(gates_t.shape, lambda i: (0, 0)),
            pl.BlockSpec((block, 2, MAIN, width), lambda i: (i, 0, 0, 0)),
        ],
        out_specs=pl.BlockSpec((count, model), lambda i: (0, 0)),
        out_shape=jax.ShapeDtypeStruct((count, model), jnp.bfloat16),
        scratch_shapes=[
            pltpu.VMEM((experts, count), jnp.float32),
            pltpu.VMEM((experts, count), jnp.float32),
            pltpu.VMEM((count, model), jnp.float32),
        ],
        cost_estimate=pl.CostEstimate(
            flops=4 * experts * CAP * count * model, bytes_accessed=4 * experts * CAP * model,
            transcendentals=0,
        ),
        name="combine_rows",
    )(ids_t, gates_t, returned)


def per_device(tokens, expert_ids, gate_weights, w_gate, w_up, w_down):
    devices = lax.axis_size("grp") * lax.axis_size("loc")
    experts = devices // 2
    ids_t = expert_ids.T
    gates_t = gate_weights.astype(jnp.float32).T
    exchange = functools.partial(
        lax.all_to_all, axis_name=AXES, split_axis=0, concat_axis=0, tiled=True
    )
    outgoing = dispatch(ids_t, tokens, experts)
    arrived = exchange(outgoing.reshape((devices,) + outgoing.shape[2:]))
    returned = exchange(half_ffn(arrived, w_gate, w_up, w_down))
    return combine(ids_t, gates_t, returned.reshape(outgoing.shape))


def solution(mesh):
    rows = P(AXES, None)
    weights = P(AXES, None, None)
    return jax.shard_map(
        per_device,
        mesh=mesh,
        in_specs=(rows, rows, rows, weights, weights, weights),
        out_specs=rows,
        check_vma=False,
    )
```

```python
import functools

import jax
import jax.numpy as jnp
from jax import lax
from jax.experimental import pallas as pl
from jax.experimental.pallas import tpu as pltpu
from jax.sharding import Mesh, PartitionSpec as P

AXES = ("grp", "x", "y")
PLANE = ("grp", "x")
CAP = 18
MAIN = 16
PIECES = 8
TILE = MAIN * PIECES
RING = 4


def split_matrix():
    row = lax.broadcasted_iota(jnp.int32, (TILE, TILE), 0)
    col = lax.broadcasted_iota(jnp.int32, (TILE, TILE), 1)
    source = (row % MAIN) // 2 * MAIN + (row % 2) * PIECES + row // MAIN
    return (source == col).astype(jnp.bfloat16)


def exact_dot(a, b, dims=((1,), (0,))):
    return lax.dot_general(a, b, (dims, ((), ())), preferred_element_type=jnp.float32)


def pieces_to_rows(pieces, matrix):
    tiles = []
    for tile in range(pieces.shape[0] // TILE):
        stacked = exact_dot(matrix, pieces[TILE * tile : TILE * (tile + 1)])
        stacked = stacked.astype(jnp.bfloat16)
        tiles.append(
            jnp.concatenate([stacked[MAIN * q : MAIN * (q + 1)] for q in range(PIECES)], axis=1)
        )
    return jnp.concatenate(tiles, axis=0)


def rows_to_pieces(rows, matrix):
    width = rows.shape[1] // PIECES
    tiles = []
    for tile in range(rows.shape[0] // MAIN):
        part = rows[MAIN * tile : MAIN * (tile + 1)]
        stacked = jnp.concatenate(
            [part[:, width * q : width * (q + 1)] for q in range(PIECES)], axis=0
        )
        tiles.append(exact_dot(matrix, stacked, ((0,), (0,))).astype(jnp.bfloat16))
    return jnp.concatenate(tiles, axis=0)


def slots_of(ids_t, expert, gates_t=None):
    count = ids_t.shape[1]
    used = jnp.zeros(expert.shape, jnp.float32)
    weight = jnp.zeros(expert.shape, jnp.float32)
    for k in range(ids_t.shape[0]):
        hit = expert == ids_t[k : k + 1, :]
        used = jnp.where(hit, 1.0, used)
        if gates_t is not None:
            weight = jnp.where(hit, gates_t[k : k + 1, :], weight)
    earlier = lax.broadcasted_iota(jnp.int32, (count, count), 0)
    later = lax.broadcasted_iota(jnp.int32, (count, count), 1)
    before = exact_dot(used.astype(jnp.bfloat16), (earlier < later).astype(jnp.bfloat16))
    return jnp.where(used > 0.0, before, -1.0), weight


def near_first(rows, count, pair):
    row = lax.broadcasted_iota(jnp.int32, (rows, count), 0)
    other = row % 2
    return row - other + jnp.where(other == 0, pair, 1 - pair)


def own_pair(rows, count, pair):
    return 2 * lax.broadcasted_iota(jnp.int32, (rows, count), 0) + pair


def pick_rows(slot, tokens):
    block, count = slot.shape
    model = tokens.shape[1]
    main_id = lax.broadcasted_iota(jnp.int32, (block, MAIN, count), 1).astype(jnp.float32)
    pick = (slot[:, None, :] == main_id).astype(jnp.float32).reshape(block * MAIN, count)
    rows = exact_dot(pick.astype(jnp.bfloat16), tokens).astype(jnp.bfloat16)
    row = lax.broadcasted_iota(jnp.int32, (2 * block, count), 0)
    slot_twice = jnp.broadcast_to(slot[:, None, :], (block, 2, count)).reshape(2 * block, count)
    pick_last = (slot_twice == (MAIN + row % 2).astype(jnp.float32)).astype(jnp.bfloat16)
    last = exact_dot(pick_last, tokens).astype(jnp.bfloat16)
    pieces = rows_to_pieces(last, split_matrix())
    return rows.reshape(block, MAIN, model), pieces.reshape(block, MAIN, model // PIECES)


def combine_rows(slot, weight, main, pieces):
    block, count = slot.shape

    def spread(first, slots):
        shape = (block, slots, count)
        slot_id = first + lax.broadcasted_iota(jnp.int32, shape, 1)
        hit = slot[:, None, :] == slot_id.astype(jnp.float32)
        scaled = jnp.where(hit, jnp.broadcast_to(weight[:, None, :], shape), 0.0)
        return scaled.reshape(block * slots, count).astype(jnp.bfloat16)

    total = exact_dot(spread(0, MAIN), main, ((0,), (0,)))
    last = pieces_to_rows(pieces, split_matrix())
    return total + exact_dot(spread(MAIN, CAP - MAIN), last, ((0,), (0,)))


def late_dispatch_kernel(pair_ref, ids_ref, tokens_ref, out_ref, slot_ref):
    block, _, _ = out_ref.shape
    model = tokens_ref.shape[1]
    step = pl.program_id(0)

    @pl.when(step == 0)
    def _():
        expert = near_first(*slot_ref.shape, pair_ref[0])
        slot_ref[...] = slots_of(ids_ref[...], expert)[0]

    slot = slot_ref[pl.ds(pl.multiple_of(step * block, block), block), :]
    rows, pieces = pick_rows(slot, tokens_ref[...])
    out_ref[:, :, :model] = rows
    out_ref[:, :, model:] = pieces


def late_dispatch(pair, ids_t, tokens, experts):
    count, model = tokens.shape
    half = model // 2
    width = half * CAP // MAIN
    block = 16
    return pl.pallas_call(
        late_dispatch_kernel,
        grid=(experts // block,),
        in_specs=[
            pl.BlockSpec(memory_space=pltpu.SMEM),
            pl.BlockSpec(ids_t.shape, lambda i: (0, 0)),
            pl.BlockSpec((count, half), lambda i: (0, 0)),
        ],
        out_specs=pl.BlockSpec((block, MAIN, width), lambda i: (i, 0, 0)),
        out_shape=jax.ShapeDtypeStruct((experts, MAIN, width), jnp.bfloat16),
        scratch_shapes=[pltpu.VMEM((experts, count), jnp.float32)],
        cost_estimate=pl.CostEstimate(
            flops=2 * experts * CAP * count * half,
            bytes_accessed=2 * experts * MAIN * width,
            transcendentals=0,
        ),
        name="late_dispatch",
    )(pair, ids_t, tokens)


def early_dispatch_kernel(pair_ref, ids_ref, tokens_ref, out_ref):
    chunks = out_ref.shape[0]
    _, count, model = tokens_ref.shape
    expert = own_pair(chunks, count, pair_ref[0])
    slot = slots_of(ids_ref[0], expert)[0]
    rows, pieces = pick_rows(slot, tokens_ref[0])
    out_ref[:, 0, :, :model] = rows
    out_ref[:, 0, :, model:] = pieces


def early_dispatch(pair, ids_t, tokens, chunks):
    ring, count, half = tokens.shape
    width = half * CAP // MAIN
    return pl.pallas_call(
        early_dispatch_kernel,
        grid=(ring,),
        in_specs=[
            pl.BlockSpec(memory_space=pltpu.SMEM),
            pl.BlockSpec((1,) + ids_t.shape[1:], lambda i: (i, 0, 0)),
            pl.BlockSpec((1, count, half), lambda i: (i, 0, 0)),
        ],
        out_specs=pl.BlockSpec((chunks, 1, MAIN, width), lambda i: (0, i, 0, 0)),
        out_shape=jax.ShapeDtypeStruct((chunks, ring, MAIN, width), jnp.bfloat16),
        cost_estimate=pl.CostEstimate(
            flops=2 * ring * chunks * CAP * count * half,
            bytes_accessed=2 * ring * chunks * MAIN * width,
            transcendentals=0,
        ),
        name="early_dispatch",
    )(pair, ids_t, tokens)


def ffn_kernel(*refs):
    late_in, (early_in, gate_ref, up_ref, down_ref) = refs[:RING], refs[RING : RING + 4]
    late_out, early_out, rows_ref = refs[RING + 4 : 2 * RING + 4], refs[-2], refs[-1]
    chunks, _, width = late_in[0].shape
    half = width * MAIN // CAP
    main = chunks * MAIN
    step = pl.program_id(0)
    matrix = split_matrix()

    def unpack(block, at):
        rows_ref[:main, at : at + half] = block[:, :, :half].reshape(main, half)
        rows_ref[main:, at : at + half] = pieces_to_rows(
            block[:, :, half:].reshape(main, width - half), matrix
        )

    def pack(value, ref, *index):
        ref[(slice(None), *index, slice(None), slice(0, half))] = value[:main].reshape(
            chunks, MAIN, half
        )
        ref[(slice(None), *index, slice(None), slice(half, None))] = rows_to_pieces(
            value[main:], matrix
        ).reshape(chunks, MAIN, width - half)

    for j in range(RING):

        @pl.when(step == j)
        def _(j=j):
            unpack(late_in[j][...], 0)

    unpack(early_in[:, 0], half)
    rows = rows_ref[...]
    gate = exact_dot(rows, gate_ref[0])
    up = exact_dot(rows, up_ref[0])
    hidden = (gate / (1.0 + jnp.exp(-gate)) * up).astype(jnp.bfloat16)
    half_out = exact_dot(hidden, down_ref[0]).astype(jnp.bfloat16)
    for j in range(RING):

        @pl.when(step == j)
        def _(j=j):
            pack(half_out[:, :half], late_out[j])

    pack(half_out[:, half:], early_out, 0)


def half_ffn(late, early, w_gate, w_up, w_down):
    chunks, _, width = late[0].shape
    model, hidden = w_gate.shape[1:]
    rows = RING * chunks * CAP
    once = pl.Buffered(1)
    late_spec = pl.BlockSpec(late[0].shape, lambda i: (0, 0, 0), pipeline_mode=once)
    early_spec = pl.BlockSpec((chunks, 1, MAIN, width), lambda i: (0, i, 0, 0))
    weights = [
        pl.BlockSpec(w.shape, lambda i: (0, 0, 0), pipeline_mode=once)
        for w in (w_gate, w_up, w_down)
    ]
    late_shape = jax.ShapeDtypeStruct(late[0].shape, jnp.bfloat16)
    *late_out, early_out = pl.pallas_call(
        ffn_kernel,
        grid=(RING,),
        in_specs=[late_spec] * RING + [early_spec] + weights,
        out_specs=[late_spec] * RING + [early_spec],
        out_shape=[late_shape] * RING + [jax.ShapeDtypeStruct(early.shape, jnp.bfloat16)],
        scratch_shapes=[pltpu.VMEM((chunks * CAP, model), jnp.bfloat16)],
        cost_estimate=pl.CostEstimate(
            flops=6 * rows * model * hidden,
            bytes_accessed=4 * rows * model + 6 * model * hidden,
            transcendentals=rows * hidden,
        ),
        compiler_params=pltpu.CompilerParams(vmem_limit_bytes=56 * 1024 * 1024),
        name="half_ffn",
    )(*late, early, w_gate, w_up, w_down)
    return late_out, early_out


def sum_halves_kernel(a_ref, b_ref, c_ref, d_ref, out_ref):
    for r, (first, second) in enumerate(((a_ref, b_ref), (c_ref, d_ref))):
        both = first[...].astype(jnp.float32) + second[...].astype(jnp.float32)
        out_ref[:, r] = both.astype(jnp.bfloat16)


def sum_halves(arrays):
    chunks, _, width = arrays[0].shape
    block = 8
    return pl.pallas_call(
        sum_halves_kernel,
        grid=(chunks // block,),
        in_specs=[pl.BlockSpec((block, MAIN, width), lambda i: (i, 0, 0))] * RING,
        out_specs=pl.BlockSpec((block, 2, MAIN, width), lambda i: (i, 0, 0, 0)),
        out_shape=jax.ShapeDtypeStruct((chunks, 2, MAIN, width), jnp.bfloat16),
        cost_estimate=pl.CostEstimate(
            flops=4 * chunks * MAIN * width, bytes_accessed=12 * chunks * MAIN * width,
            transcendentals=0,
        ),
        name="sum_halves",
    )(*arrays)


def early_combine_kernel(pair_ref, ids_ref, gates_ref, rows_ref, out_ref):
    chunks = rows_ref.shape[0]
    _, count, half = out_ref.shape
    expert = own_pair(chunks, count, pair_ref[0])
    slot, weight = slots_of(ids_ref[0], expert, gates_ref[0])
    main = rows_ref[:, 0, :, :half].reshape(chunks * MAIN, half)
    pieces = rows_ref[:, 0, :, half:].reshape(chunks * MAIN, half // PIECES)
    out_ref[0] = combine_rows(slot, weight, main, pieces).astype(jnp.bfloat16)


def early_combine(pair, ids_t, gates_t, rows):
    chunks, ring, _, width = rows.shape
    count = ids_t.shape[2]
    half = width * MAIN // CAP
    return pl.pallas_call(
        early_combine_kernel,
        grid=(ring,),
        in_specs=[
            pl.BlockSpec(memory_space=pltpu.SMEM),
            pl.BlockSpec((1,) + ids_t.shape[1:], lambda i: (i, 0, 0)),
            pl.BlockSpec((1,) + gates_t.shape[1:], lambda i: (i, 0, 0)),
            pl.BlockSpec((chunks, 1, MAIN, width), lambda i: (0, i, 0, 0)),
        ],
        out_specs=pl.BlockSpec((1, count, half), lambda i: (i, 0, 0)),
        out_shape=jax.ShapeDtypeStruct((ring, count, half), jnp.bfloat16),
        cost_estimate=pl.CostEstimate(
            flops=2 * ring * chunks * CAP * count * half,
            bytes_accessed=2 * ring * chunks * MAIN * width,
            transcendentals=0,
        ),
        name="early_combine",
    )(pair, ids_t, gates_t, rows)


def final_kernel(pair_ref, ids_ref, gates_ref, rows_ref, *refs):
    parts, (out_ref, slot_ref, weight_ref, acc_ref) = refs[:RING], refs[RING:]
    block = rows_ref.shape[0]
    half = acc_ref.shape[1]
    step = pl.program_id(0)

    @pl.when(step == 0)
    def _():
        expert = near_first(*slot_ref.shape, pair_ref[0])
        slot, weight = slots_of(ids_ref[...], expert, gates_ref[...])
        slot_ref[...] = slot
        weight_ref[...] = weight
        acc_ref[...] = jnp.zeros_like(acc_ref)

    here = pl.ds(pl.multiple_of(step * block, block), block)
    main = rows_ref[:, :, :half].reshape(block * MAIN, half)
    pieces = rows_ref[:, :, half:].reshape(block * MAIN, half // PIECES)
    acc_ref[...] += combine_rows(slot_ref[here, :], weight_ref[here, :], main, pieces)

    @pl.when(step == pl.num_programs(0) - 1)
    def _():
        out_ref[:, :half] = acc_ref[...].astype(jnp.bfloat16)
        total = parts[0][...].astype(jnp.float32)
        for part in parts[1:]:
            total += part[...].astype(jnp.float32)
        out_ref[:, half:] = total.astype(jnp.bfloat16)


def final_combine(pair, ids_t, gates_t, rows, parts):
    experts, _, width = rows.shape
    count, half = parts[0].shape
    block = 16
    whole = lambda i: (0, 0)
    return pl.pallas_call(
        final_kernel,
        grid=(experts // block,),
        in_specs=[
            pl.BlockSpec(memory_space=pltpu.SMEM),
            pl.BlockSpec(ids_t.shape, whole),
            pl.BlockSpec(gates_t.shape, whole),
            pl.BlockSpec((block, MAIN, width), lambda i: (i, 0, 0)),
        ]
        + [pl.BlockSpec((count, half), whole)] * RING,
        out_specs=pl.BlockSpec((count, 2 * half), whole),
        out_shape=jax.ShapeDtypeStruct((count, 2 * half), jnp.bfloat16),
        scratch_shapes=[
            pltpu.VMEM((experts, count), jnp.float32),
            pltpu.VMEM((experts, count), jnp.float32),
            pltpu.VMEM((count, half), jnp.float32),
        ],
        cost_estimate=pl.CostEstimate(
            flops=2 * experts * CAP * count * half,
            bytes_accessed=2 * experts * MAIN * width,
            transcendentals=0,
        ),
        name="final_combine",
    )(pair, ids_t, gates_t, rows, *parts)


def across(array, j):
    return lax.ppermute(array, "y", [(y, y ^ j) for y in range(RING)])


def gather_ring(array):
    return jnp.stack([array] + [across(array, j) for j in range(1, RING)])


def plane_exchange(array):
    return lax.all_to_all(array, PLANE, split_axis=0, concat_axis=0, tiled=True)


def per_device(tokens, expert_ids, gate_weights, w_gate, w_up, w_down):
    chunks = lax.axis_size("grp") * lax.axis_size("x")
    experts = 2 * chunks
    top = expert_ids.shape[1]
    half = tokens.shape[1] // 2
    pair = (lax.axis_index("y") // 2).astype(jnp.int32).reshape(1)
    ids_t = expert_ids.T
    gates_t = gate_weights.T

    late = late_dispatch(pair, ids_t, tokens, experts)
    width = late.shape[2]
    late = plane_exchange(late.reshape(chunks, 2 * MAIN, width))
    late = late.reshape(chunks, 2, MAIN, width)
    near, far = late[:, 0], late[:, 1]

    routing = gather_ring(jnp.concatenate([ids_t.astype(jnp.bfloat16), gates_t], axis=0))
    ids_ring = routing[:, :top].astype(jnp.int32)
    gates_ring = routing[:, top:].astype(jnp.float32)
    early = early_dispatch(pair, ids_ring, gather_ring(tokens[:, half:]), chunks)
    early = plane_exchange(early.reshape(chunks, RING * MAIN, width))
    early = early.reshape(chunks, RING, MAIN, width)

    late_in = (near, across(near, 1), across(far, 2), across(far, 3))
    late_out, early_out = half_ffn(late_in, early, w_gate, w_up, w_down)

    early_out = plane_exchange(early_out.reshape(chunks, RING * MAIN, width))
    late_back = [late_out[0]] + [across(late_out[j], j) for j in range(1, RING)]
    late_back = plane_exchange(sum_halves(late_back).reshape(chunks, 2 * MAIN, width))
    partial = early_combine(
        pair, ids_ring, gates_ring, early_out.reshape(chunks, RING, MAIN, width)
    )
    parts = [partial[0]] + [across(partial[j], j) for j in range(1, RING)]
    return final_combine(
        pair, ids_t, gates_t.astype(jnp.float32), late_back.reshape(experts, MAIN, width), parts
    )


def solution(mesh):
    ring = Mesh(mesh.devices.reshape(mesh.devices.shape[0], -1, RING), AXES)
    rows = P(AXES, None)
    weights = P(AXES, None, None)
    return jax.shard_map(
        per_device,
        mesh=ring,
        in_specs=(rows, rows, rows, weights, weights, weights),
        out_specs=rows,
        check_vma=False,
    )
```

```python
import jax
import jax.numpy as jnp
from jax import lax
from jax.experimental import pallas as pl
from jax.experimental.pallas import tpu as pltpu
from jax.sharding import Mesh, PartitionSpec as P

AXES = ("grp", "x", "y")
PLANE = ("grp", "x")
CAP = 18
MAIN = 16
PIECES = 8
TILE = MAIN * PIECES
RING = 4
ORDER = (2, 1, 3, 0)


def split_matrix():
    row = lax.broadcasted_iota(jnp.int32, (TILE, TILE), 0)
    col = lax.broadcasted_iota(jnp.int32, (TILE, TILE), 1)
    source = (row % MAIN) // 2 * MAIN + (row % 2) * PIECES + row // MAIN
    return (source == col).astype(jnp.bfloat16)


def exact_dot(a, b, dims=((1,), (0,))):
    return lax.dot_general(a, b, (dims, ((), ())), preferred_element_type=jnp.float32)


def pieces_to_rows(pieces, matrix):
    tiles = []
    for tile in range(pieces.shape[0] // TILE):
        stacked = exact_dot(matrix, pieces[TILE * tile : TILE * (tile + 1)])
        stacked = stacked.astype(jnp.bfloat16)
        tiles.append(
            jnp.concatenate([stacked[MAIN * q : MAIN * (q + 1)] for q in range(PIECES)], axis=1)
        )
    return jnp.concatenate(tiles, axis=0)


def rows_to_pieces(rows, matrix):
    width = rows.shape[1] // PIECES
    tiles = []
    for tile in range(rows.shape[0] // MAIN):
        part = rows[MAIN * tile : MAIN * (tile + 1)]
        stacked = jnp.concatenate(
            [part[:, width * q : width * (q + 1)] for q in range(PIECES)], axis=0
        )
        tiles.append(exact_dot(matrix, stacked, ((0,), (0,))).astype(jnp.bfloat16))
    return jnp.concatenate(tiles, axis=0)


def slots_of(ids_t, expert, gates_t=None):
    count = ids_t.shape[1]
    used = jnp.zeros(expert.shape, jnp.float32)
    weight = jnp.zeros(expert.shape, jnp.float32)
    for k in range(ids_t.shape[0]):
        hit = expert == ids_t[k : k + 1, :]
        used = jnp.where(hit, 1.0, used)
        if gates_t is not None:
            weight = jnp.where(hit, gates_t[k : k + 1, :], weight)
    earlier = lax.broadcasted_iota(jnp.int32, (count, count), 0)
    later = lax.broadcasted_iota(jnp.int32, (count, count), 1)
    before = exact_dot(used.astype(jnp.bfloat16), (earlier < later).astype(jnp.bfloat16))
    return jnp.where(used > 0.0, before, -1.0), weight


def near_first(rows, count, pair):
    row = lax.broadcasted_iota(jnp.int32, (rows, count), 0)
    other = row % 2
    return row - other + jnp.where(other == 0, pair, 1 - pair)


def own_pair(rows, count, pair):
    return 2 * lax.broadcasted_iota(jnp.int32, (rows, count), 0) + pair


def pick_rows(slot, tokens):
    block, count = slot.shape
    model = tokens.shape[1]
    main_id = lax.broadcasted_iota(jnp.int32, (block, MAIN, count), 1).astype(jnp.float32)
    pick = (slot[:, None, :] == main_id).astype(jnp.float32).reshape(block * MAIN, count)
    rows = exact_dot(pick.astype(jnp.bfloat16), tokens).astype(jnp.bfloat16)
    row = lax.broadcasted_iota(jnp.int32, (2 * block, count), 0)
    slot_twice = jnp.broadcast_to(slot[:, None, :], (block, 2, count)).reshape(2 * block, count)
    pick_last = (slot_twice == (MAIN + row % 2).astype(jnp.float32)).astype(jnp.bfloat16)
    last = exact_dot(pick_last, tokens).astype(jnp.bfloat16)
    pieces = rows_to_pieces(last, split_matrix())
    return rows.reshape(block, MAIN, model), pieces.reshape(block, MAIN, model // PIECES)


def combine_rows(slot, weight, main, pieces):
    block, count = slot.shape

    def spread(first, slots):
        shape = (block, slots, count)
        slot_id = first + lax.broadcasted_iota(jnp.int32, shape, 1)
        hit = slot[:, None, :] == slot_id.astype(jnp.float32)
        scaled = jnp.where(hit, jnp.broadcast_to(weight[:, None, :], shape), 0.0)
        return scaled.reshape(block * slots, count).astype(jnp.bfloat16)

    total = exact_dot(spread(0, MAIN), main, ((0,), (0,)))
    last = pieces_to_rows(pieces, split_matrix())
    return total + exact_dot(spread(MAIN, CAP - MAIN), last, ((0,), (0,)))


def late_dispatch_kernel(pair_ref, ids_ref, tokens_ref, out_ref, slot_ref):
    block, _, _ = out_ref.shape
    model = tokens_ref.shape[1]
    step = pl.program_id(0)

    @pl.when(step == 0)
    def _():
        expert = near_first(*slot_ref.shape, pair_ref[0])
        slot_ref[...] = slots_of(ids_ref[...], expert)[0]

    slot = slot_ref[pl.ds(pl.multiple_of(step * block, block), block), :]
    rows, pieces = pick_rows(slot, tokens_ref[...])
    out_ref[:, :, :model] = rows
    out_ref[:, :, model:] = pieces


def late_dispatch(pair, ids_t, tokens, experts):
    count, model = tokens.shape
    half = model // 2
    width = half * CAP // MAIN
    block = 16
    return pl.pallas_call(
        late_dispatch_kernel,
        grid=(experts // block,),
        in_specs=[
            pl.BlockSpec(memory_space=pltpu.SMEM),
            pl.BlockSpec(ids_t.shape, lambda i: (0, 0)),
            pl.BlockSpec((count, half), lambda i: (0, 0)),
        ],
        out_specs=pl.BlockSpec((block, MAIN, width), lambda i: (i, 0, 0)),
        out_shape=jax.ShapeDtypeStruct((experts, MAIN, width), jnp.bfloat16),
        scratch_shapes=[pltpu.VMEM((experts, count), jnp.float32)],
        cost_estimate=pl.CostEstimate(
            flops=2 * experts * CAP * count * half,
            bytes_accessed=2 * experts * MAIN * width,
            transcendentals=0,
        ),
        compiler_params=pltpu.CompilerParams(vmem_limit_bytes=12 * 1024 * 1024),
        name="late_dispatch",
    )(pair, ids_t, tokens)


def early_dispatch_kernel(pair_ref, ids_ref, tokens_ref, out_ref):
    chunks = out_ref.shape[0]
    _, count, model = tokens_ref.shape
    expert = own_pair(chunks, count, pair_ref[0])
    slot = slots_of(ids_ref[0], expert)[0]
    rows, pieces = pick_rows(slot, tokens_ref[0])
    out_ref[:, 0, :, :model] = rows
    out_ref[:, 0, :, model:] = pieces


def early_dispatch(pair, ids_t, tokens, chunks):
    ring, count, half = tokens.shape
    width = half * CAP // MAIN
    return pl.pallas_call(
        early_dispatch_kernel,
        grid=(ring,),
        in_specs=[
            pl.BlockSpec(memory_space=pltpu.SMEM),
            pl.BlockSpec((1,) + ids_t.shape[1:], lambda i: (i, 0, 0)),
            pl.BlockSpec((1, count, half), lambda i: (i, 0, 0)),
        ],
        out_specs=pl.BlockSpec((chunks, 1, MAIN, width), lambda i: (0, i, 0, 0)),
        out_shape=jax.ShapeDtypeStruct((chunks, ring, MAIN, width), jnp.bfloat16),
        cost_estimate=pl.CostEstimate(
            flops=2 * ring * chunks * CAP * count * half,
            bytes_accessed=2 * ring * chunks * MAIN * width,
            transcendentals=0,
        ),
        compiler_params=pltpu.CompilerParams(vmem_limit_bytes=12 * 1024 * 1024),
        name="early_dispatch",
    )(pair, ids_t, tokens)


def unpack_chunks(block, rows_ref, matrix):
    chunks, _, width = block.shape
    half = rows_ref.shape[1]
    main = chunks * MAIN
    rows_ref[:main, :] = block[:, :, :half].reshape(main, half)
    rows_ref[main:, :] = pieces_to_rows(block[:, :, half:].reshape(main, width - half), matrix)


def pack_chunks(value, matrix):
    half = value.shape[1]
    chunks = value.shape[0] // CAP
    main = chunks * MAIN
    pieces = rows_to_pieces(value[main:], matrix).reshape(chunks, MAIN, half // PIECES)
    return value[:main].reshape(chunks, MAIN, half), pieces


def first_ffn_kernel(late_ref, gate_ref, up_ref, gate_out, up_out, rows_ref):
    half = rows_ref.shape[1]
    unpack_chunks(late_ref[...], rows_ref, split_matrix())
    rows = rows_ref[...]
    gate_out[...] = exact_dot(rows, gate_ref[0, :half, :])
    up_out[...] = exact_dot(rows, up_ref[0, :half, :])


def first_ffn(late, w_gate, w_up):
    chunks, _, _ = late.shape
    model, hidden = w_gate.shape[1:]
    rows = chunks * CAP
    half = model // 2
    on_chip = pl.BlockSpec(memory_space=pltpu.VMEM)
    out = jax.ShapeDtypeStruct((rows, hidden), jnp.float32)
    return pl.pallas_call(
        first_ffn_kernel,
        in_specs=[on_chip] * 3,
        out_specs=[on_chip] * 2,
        out_shape=[out, out],
        scratch_shapes=[pltpu.VMEM((rows, half), jnp.bfloat16)],
        cost_estimate=pl.CostEstimate(
            flops=4 * rows * half * hidden, bytes_accessed=8 * rows * hidden, transcendentals=0
        ),
        compiler_params=pltpu.CompilerParams(vmem_limit_bytes=12 * 1024 * 1024),
        name="first_ffn",
    )(late, w_gate, w_up)


def second_ffn_kernel(early_ref, gate_in, up_in, gate_ref, up_ref, down_ref, *refs):
    late_out, early_out, rows_ref = refs[-3:]
    half = rows_ref.shape[1]
    matrix = split_matrix()
    unpack_chunks(early_ref[:, 0], rows_ref, matrix)
    rows = rows_ref[...]
    gate = gate_in[...] + exact_dot(rows, gate_ref[0, half:, :])
    up = up_in[...] + exact_dot(rows, up_ref[0, half:, :])
    hidden = (gate / (1.0 + jnp.exp(-gate)) * up).astype(jnp.bfloat16)
    value = exact_dot(hidden, down_ref[0, :, :half]).astype(jnp.bfloat16)
    main, pieces = pack_chunks(value, matrix)
    late_out[:, :, :half] = main
    late_out[:, :, half:] = pieces
    value = exact_dot(hidden, down_ref[0, :, half:]).astype(jnp.bfloat16)
    main, pieces = pack_chunks(value, matrix)
    early_out[:, 0, :, :half] = main
    early_out[:, 0, :, half:] = pieces


def second_ffn(j, early, gate, up, w_gate, w_up, w_down, early_out):
    chunks, _, _, width = early.shape
    model, hidden = w_gate.shape[1:]
    rows = chunks * CAP
    half = model // 2
    on_chip = pl.BlockSpec(memory_space=pltpu.VMEM)
    block = pl.BlockSpec((chunks, 1, MAIN, width), lambda i: (0, j, 0, 0))
    held = [] if early_out is None else [early_out]
    return pl.pallas_call(
        second_ffn_kernel,
        grid=(1,),
        in_specs=[block] + [on_chip] * 5 + [pl.BlockSpec(memory_space=pl.ANY)] * len(held),
        out_specs=[on_chip, block],
        out_shape=[
            jax.ShapeDtypeStruct((chunks, MAIN, width), jnp.bfloat16),
            pltpu.HBM(early.shape, jnp.bfloat16),
        ],
        input_output_aliases={6: 1} if held else {},
        scratch_shapes=[pltpu.VMEM((rows, half), jnp.bfloat16)],
        cost_estimate=pl.CostEstimate(
            flops=2 * rows * model * hidden + 4 * rows * half * hidden,
            bytes_accessed=4 * rows * half + 8 * rows * hidden,
            transcendentals=rows * hidden,
        ),
        compiler_params=pltpu.CompilerParams(vmem_limit_bytes=20 * 1024 * 1024),
        name="second_ffn",
    )(early, gate, up, w_gate, w_up, w_down, *held)


def sum_halves_kernel(a_ref, b_ref, c_ref, d_ref, out_ref):
    for r, (first, second) in enumerate(((a_ref, b_ref), (c_ref, d_ref))):
        for i in range(0, first.shape[0], 8):
            both = first[i : i + 8].astype(jnp.float32) + second[i : i + 8].astype(jnp.float32)
            out_ref[i : i + 8, r] = both.astype(jnp.bfloat16)


def sum_halves(arrays):
    chunks, _, width = arrays[0].shape
    on_chip = pl.BlockSpec(memory_space=pltpu.VMEM)
    return pl.pallas_call(
        sum_halves_kernel,
        in_specs=[on_chip] * RING,
        out_specs=on_chip,
        out_shape=jax.ShapeDtypeStruct((chunks, 2, MAIN, width), jnp.bfloat16),
        cost_estimate=pl.CostEstimate(
            flops=4 * chunks * MAIN * width, bytes_accessed=12 * chunks * MAIN * width,
            transcendentals=0,
        ),
        compiler_params=pltpu.CompilerParams(vmem_limit_bytes=12 * 1024 * 1024),
        name="sum_halves",
    )(*arrays)


def early_combine_kernel(pair_ref, ids_ref, gates_ref, rows_ref, out_ref):
    chunks = rows_ref.shape[0]
    _, count, half = out_ref.shape
    expert = own_pair(chunks, count, pair_ref[0])
    slot, weight = slots_of(ids_ref[0], expert, gates_ref[0])
    main = rows_ref[:, 0, :, :half].reshape(chunks * MAIN, half)
    pieces = rows_ref[:, 0, :, half:].reshape(chunks * MAIN, half // PIECES)
    out_ref[0] = combine_rows(slot, weight, main, pieces).astype(jnp.bfloat16)


def early_combine(pair, ids_t, gates_t, rows):
    chunks, ring, _, width = rows.shape
    count = ids_t.shape[2]
    half = width * MAIN // CAP
    return pl.pallas_call(
        early_combine_kernel,
        grid=(ring,),
        in_specs=[
            pl.BlockSpec(memory_space=pltpu.SMEM),
            pl.BlockSpec((1,) + ids_t.shape[1:], lambda i: (i, 0, 0)),
            pl.BlockSpec((1,) + gates_t.shape[1:], lambda i: (i, 0, 0)),
            pl.BlockSpec((chunks, 1, MAIN, width), lambda i: (0, i, 0, 0)),
        ],
        out_specs=pl.BlockSpec((1, count, half), lambda i: (i, 0, 0)),
        out_shape=jax.ShapeDtypeStruct((ring, count, half), jnp.bfloat16),
        cost_estimate=pl.CostEstimate(
            flops=2 * ring * chunks * CAP * count * half,
            bytes_accessed=2 * ring * chunks * MAIN * width,
            transcendentals=0,
        ),
        compiler_params=pltpu.CompilerParams(vmem_limit_bytes=12 * 1024 * 1024),
        name="early_combine",
    )(pair, ids_t, gates_t, rows)


def final_kernel(pair_ref, ids_ref, gates_ref, rows_ref, *refs):
    parts, (out_ref, slot_ref, weight_ref) = refs[:RING], refs[RING:]
    experts = rows_ref.shape[0]
    half = parts[0].shape[1]
    block = 16
    expert = near_first(*slot_ref.shape, pair_ref[0])
    slot, weight = slots_of(ids_ref[...], expert, gates_ref[...])
    slot_ref[...] = slot
    weight_ref[...] = weight
    total = jnp.zeros((slot.shape[1], half), jnp.float32)
    for first in range(0, experts, block):
        here = slice(first, first + block)
        main = rows_ref[here, :, :half].reshape(block * MAIN, half)
        pieces = rows_ref[here, :, half:].reshape(block * MAIN, half // PIECES)
        total += combine_rows(slot_ref[here, :], weight_ref[here, :], main, pieces)
    out_ref[:, :half] = total.astype(jnp.bfloat16)
    total = parts[0][...].astype(jnp.float32)
    for part in parts[1:]:
        total += part[...].astype(jnp.float32)
    out_ref[:, half:] = total.astype(jnp.bfloat16)


def final_combine(pair, ids_t, gates_t, rows, parts):
    experts, _, width = rows.shape
    count, half = parts[0].shape
    on_chip = pl.BlockSpec(memory_space=pltpu.VMEM)
    return pl.pallas_call(
        final_kernel,
        in_specs=[pl.BlockSpec(memory_space=pltpu.SMEM)] + [on_chip] * (3 + RING),
        out_specs=on_chip,
        out_shape=jax.ShapeDtypeStruct((count, 2 * half), jnp.bfloat16),
        scratch_shapes=[
            pltpu.VMEM((experts, count), jnp.float32),
            pltpu.VMEM((experts, count), jnp.float32),
        ],
        cost_estimate=pl.CostEstimate(
            flops=2 * experts * CAP * count * half,
            bytes_accessed=2 * experts * MAIN * width,
            transcendentals=0,
        ),
        compiler_params=pltpu.CompilerParams(vmem_limit_bytes=16 * 1024 * 1024),
        name="final_combine",
    )(pair, ids_t, gates_t, rows, *parts)


def across(array, j):
    return lax.ppermute(array, "y", [(y, y ^ j) for y in range(RING)])


def gather_ring(array):
    return jnp.stack([array] + [across(array, j) for j in range(1, RING)])


def plane_exchange(array):
    return lax.all_to_all(array, PLANE, split_axis=0, concat_axis=0, tiled=True)


def per_device(tokens, expert_ids, gate_weights, w_gate, w_up, w_down):
    chunks = lax.axis_size("grp") * lax.axis_size("x")
    experts = 2 * chunks
    top = expert_ids.shape[1]
    half = tokens.shape[1] // 2
    pair = (lax.axis_index("y") // 2).astype(jnp.int32).reshape(1)
    ids_t = expert_ids.T
    gates_t = gate_weights.T

    late = late_dispatch(pair, ids_t, tokens, experts)
    width = late.shape[2]
    late = plane_exchange(late.reshape(chunks, 2 * MAIN, width))
    late = late.reshape(chunks, 2, MAIN, width)
    near, far = late[:, 0], late[:, 1]

    routing = gather_ring(jnp.concatenate([ids_t.astype(jnp.bfloat16), gates_t], axis=0))
    ids_ring = routing[:, :top].astype(jnp.int32)
    gates_ring = routing[:, top:].astype(jnp.float32)
    early = early_dispatch(pair, ids_ring, gather_ring(tokens[:, half:]), chunks)
    early = plane_exchange(early.reshape(chunks, RING * MAIN, width))
    early = early.reshape(chunks, RING, MAIN, width)

    late_in = (near, across(near, 1), across(far, 2), across(far, 3))
    first = {j: first_ffn(late_in[j], w_gate, w_up) for j in (0, 1, 3, 2)}
    early_out, late_back = None, [None] * RING
    for j in ORDER:
        late_out, early_out = second_ffn(j, early, *first[j], w_gate, w_up, w_down, early_out)
        late_back[j] = across(late_out, j) if j else late_out

    early_out = plane_exchange(early_out.reshape(chunks, RING * MAIN, width))
    late_back = plane_exchange(sum_halves(late_back).reshape(chunks, 2 * MAIN, width))
    partial = early_combine(
        pair, ids_ring, gates_ring, early_out.reshape(chunks, RING, MAIN, width)
    )
    parts = [partial[0]] + [across(partial[j], j) for j in range(1, RING)]
    return final_combine(
        pair, ids_t, gates_t.astype(jnp.float32), late_back.reshape(experts, MAIN, width), parts
    )


def solution(mesh):
    ring = Mesh(mesh.devices.reshape(mesh.devices.shape[0], -1, RING), AXES)
    rows = P(AXES, None)
    weights = P(AXES, None, None)

    return jax.shard_map(
        per_device,
        mesh=ring,
        in_specs=(rows, rows, rows, weights, weights, weights),
        out_specs=rows,
        check_vma=False,
    )
```

```python
import jax
import jax.numpy as jnp
from jax import lax
from jax.experimental import pallas as pl
from jax.experimental.pallas import tpu as pltpu
from jax.sharding import Mesh, PartitionSpec as P

AXES = ("grp", "x", "y")
PLANE = ("grp", "x")
CAP = 18
MAIN = 16
PIECES = 8
TILE = MAIN * PIECES
RING = 4
ORDER = (0, 1, 3, 2)


def split_matrix():
    row = lax.broadcasted_iota(jnp.int32, (TILE, TILE), 0)
    col = lax.broadcasted_iota(jnp.int32, (TILE, TILE), 1)
    source = (row % MAIN) // 2 * MAIN + (row % 2) * PIECES + row // MAIN
    return (source == col).astype(jnp.bfloat16)


def exact_dot(a, b, dims=((1,), (0,))):
    return lax.dot_general(a, b, (dims, ((), ())), preferred_element_type=jnp.float32)


def pieces_to_rows(pieces, matrix):
    tiles = []
    for tile in range(pieces.shape[0] // TILE):
        stacked = exact_dot(matrix, pieces[TILE * tile : TILE * (tile + 1)])
        stacked = stacked.astype(jnp.bfloat16)
        tiles.append(
            jnp.concatenate([stacked[MAIN * q : MAIN * (q + 1)] for q in range(PIECES)], axis=1)
        )
    return jnp.concatenate(tiles, axis=0)


def rows_to_pieces(rows, matrix):
    width = rows.shape[1] // PIECES
    tiles = []
    for tile in range(rows.shape[0] // MAIN):
        part = rows[MAIN * tile : MAIN * (tile + 1)]
        stacked = jnp.concatenate(
            [part[:, width * q : width * (q + 1)] for q in range(PIECES)], axis=0
        )
        tiles.append(exact_dot(matrix, stacked, ((0,), (0,))).astype(jnp.bfloat16))
    return jnp.concatenate(tiles, axis=0)


def slots_of(ids_t, expert, gates_t=None):
    count = ids_t.shape[1]
    used = jnp.zeros(expert.shape, jnp.float32)
    weight = jnp.zeros(expert.shape, jnp.float32)
    for k in range(ids_t.shape[0]):
        hit = expert == ids_t[k : k + 1, :]
        used = jnp.where(hit, 1.0, used)
        if gates_t is not None:
            weight = jnp.where(hit, gates_t[k : k + 1, :], weight)
    earlier = lax.broadcasted_iota(jnp.int32, (count, count), 0)
    later = lax.broadcasted_iota(jnp.int32, (count, count), 1)
    before = exact_dot(used.astype(jnp.bfloat16), (earlier < later).astype(jnp.bfloat16))
    return jnp.where(used > 0.0, before, -1.0), weight


def near_first(rows, count, pair):
    row = lax.broadcasted_iota(jnp.int32, (rows, count), 0)
    other = row % 2
    return row - other + jnp.where(other == 0, pair, 1 - pair)


def own_pair(rows, count, pair):
    return 2 * lax.broadcasted_iota(jnp.int32, (rows, count), 0) + pair


def pick_rows(slot, tokens):
    block, count = slot.shape
    model = tokens.shape[1]
    main_id = lax.broadcasted_iota(jnp.int32, (block, MAIN, count), 1).astype(jnp.float32)
    pick = (slot[:, None, :] == main_id).astype(jnp.float32).reshape(block * MAIN, count)
    rows = exact_dot(pick.astype(jnp.bfloat16), tokens).astype(jnp.bfloat16)
    row = lax.broadcasted_iota(jnp.int32, (2 * block, count), 0)
    slot_twice = jnp.broadcast_to(slot[:, None, :], (block, 2, count)).reshape(2 * block, count)
    pick_last = (slot_twice == (MAIN + row % 2).astype(jnp.float32)).astype(jnp.bfloat16)
    last = exact_dot(pick_last, tokens).astype(jnp.bfloat16)
    pieces = rows_to_pieces(last, split_matrix())
    return rows.reshape(block, MAIN, model), pieces.reshape(block, MAIN, model // PIECES)


def combine_rows(slot, weight, main, pieces):
    block, count = slot.shape

    def spread(first, slots):
        shape = (block, slots, count)
        slot_id = first + lax.broadcasted_iota(jnp.int32, shape, 1)
        hit = slot[:, None, :] == slot_id.astype(jnp.float32)
        scaled = jnp.where(hit, jnp.broadcast_to(weight[:, None, :], shape), 0.0)
        return scaled.reshape(block * slots, count).astype(jnp.bfloat16)

    total = exact_dot(spread(0, MAIN), main, ((0,), (0,)))
    last = pieces_to_rows(pieces, split_matrix())
    return total + exact_dot(spread(MAIN, CAP - MAIN), last, ((0,), (0,)))


def late_dispatch_kernel(pair_ref, ids_ref, tokens_ref, out_ref, slot_ref):
    block, _, _ = out_ref.shape
    model = tokens_ref.shape[1]
    step = pl.program_id(0)

    @pl.when(step == 0)
    def _():
        expert = near_first(*slot_ref.shape, pair_ref[0])
        slot_ref[...] = slots_of(ids_ref[...], expert)[0]

    slot = slot_ref[pl.ds(pl.multiple_of(step * block, block), block), :]
    rows, pieces = pick_rows(slot, tokens_ref[...])
    out_ref[:, :, :model] = rows
    out_ref[:, :, model:] = pieces


def late_dispatch(pair, ids_t, tokens, experts):
    count, model = tokens.shape
    half = model // 2
    width = half * CAP // MAIN
    block = 16
    return pl.pallas_call(
        late_dispatch_kernel,
        grid=(experts // block,),
        in_specs=[
            pl.BlockSpec(memory_space=pltpu.SMEM),
            pl.BlockSpec(ids_t.shape, lambda i: (0, 0)),
            pl.BlockSpec((count, half), lambda i: (0, 0)),
        ],
        out_specs=pl.BlockSpec((block, MAIN, width), lambda i: (i, 0, 0)),
        out_shape=jax.ShapeDtypeStruct((experts, MAIN, width), jnp.bfloat16),
        scratch_shapes=[pltpu.VMEM((experts, count), jnp.float32)],
        cost_estimate=pl.CostEstimate(
            flops=2 * experts * CAP * count * half,
            bytes_accessed=2 * experts * MAIN * width,
            transcendentals=0,
        ),
        compiler_params=pltpu.CompilerParams(vmem_limit_bytes=12 * 1024 * 1024),
        name="late_dispatch",
    )(pair, ids_t, tokens)


def early_dispatch_kernel(pair_ref, ids_ref, tokens_ref, out_ref):
    chunks = out_ref.shape[0]
    _, count, model = tokens_ref.shape
    expert = own_pair(chunks, count, pair_ref[0])
    slot = slots_of(ids_ref[0], expert)[0]
    rows, pieces = pick_rows(slot, tokens_ref[0])
    out_ref[:, 0, :, :model] = rows
    out_ref[:, 0, :, model:] = pieces


def early_dispatch(pair, ids_t, tokens, chunks):
    ring, count, half = tokens.shape
    width = half * CAP // MAIN
    return pl.pallas_call(
        early_dispatch_kernel,
        grid=(ring,),
        in_specs=[
            pl.BlockSpec(memory_space=pltpu.SMEM),
            pl.BlockSpec((1,) + ids_t.shape[1:], lambda i: (i, 0, 0)),
            pl.BlockSpec((1, count, half), lambda i: (i, 0, 0)),
        ],
        out_specs=pl.BlockSpec((chunks, 1, MAIN, width), lambda i: (0, i, 0, 0)),
        out_shape=jax.ShapeDtypeStruct((chunks, ring, MAIN, width), jnp.bfloat16),
        cost_estimate=pl.CostEstimate(
            flops=2 * ring * chunks * CAP * count * half,
            bytes_accessed=2 * ring * chunks * MAIN * width,
            transcendentals=0,
        ),
        compiler_params=pltpu.CompilerParams(vmem_limit_bytes=12 * 1024 * 1024),
        name="early_dispatch",
    )(pair, ids_t, tokens)


def ffn_kernel(*refs):
    late_hbm, (early_hbm, gate_hbm, up_hbm, down_hbm) = refs[:RING], refs[RING : RING + 4]
    late_out, early_out = refs[RING + 4 : 2 * RING + 4], refs[2 * RING + 4]
    late_in, early_in, gate_w, up_w, down_w, late_made, early_made, in_sems, out_sems = refs[
        2 * RING + 5 :
    ]
    _, chunks, _, width = late_in.shape
    model = gate_w.shape[0]
    half = model // 2
    main = chunks * MAIN
    last = 2 * chunks
    first, second = pl.ds(0, half), pl.ds(half, half)
    body, tail = pl.ds(0, half), pl.ds(half, width - half)

    reads = {}

    def read(name, source, target):
        reads[name] = pltpu.make_async_copy(source, target, in_sems.at[len(reads)])
        reads[name].start()

    def read_rows(j):
        read(("late", j), late_hbm[j], late_in.at[j])
        read(("early", j), early_hbm.at[:, j], early_in.at[j])

    read("gate_first", gate_hbm.at[0, first], gate_w.at[first])
    read(("late", ORDER[0]), late_hbm[ORDER[0]], late_in.at[ORDER[0]])
    read("up_first", up_hbm.at[0, first], up_w.at[first])
    read(("early", ORDER[0]), early_hbm.at[:, ORDER[0]], early_in.at[ORDER[0]])
    read("gate_second", gate_hbm.at[0, second], gate_w.at[second])
    read("up_second", up_hbm.at[0, second], up_w.at[second])
    read("down", down_hbm.at[0], down_w)
    for j in ORDER[1:]:
        read_rows(j)

    waited = set()

    def ready(*names):
        for name in names:
            if name not in waited:
                waited.add(name)
                reads[name].wait()

    writes = []

    def write(source, target):
        writes.append(pltpu.make_async_copy(source, target, out_sems.at[len(writes)]))
        writes[-1].start()

    def half_expert(late, early, j=None):
        if j is not None:
            ready("gate_first", ("late", j))
        gate = exact_dot(late(), gate_w[:half, :])
        ready("up_first")
        up = exact_dot(late(), up_w[:half, :])
        if j is not None:
            ready(("early", j), "gate_second")
        gate = gate + exact_dot(early(), gate_w[half:, :])
        ready("up_second")
        up = up + exact_dot(early(), up_w[half:, :])
        hidden = (gate / (1.0 + jnp.exp(-gate)) * up).astype(jnp.bfloat16)
        ready("down")
        late_value = exact_dot(hidden, down_w[:, :half]).astype(jnp.bfloat16)
        early_value = exact_dot(hidden, down_w[:, half:]).astype(jnp.bfloat16)
        return late_value, early_value

    for j in ORDER:
        late_value, early_value = half_expert(
            lambda: late_in[j, :, :, :half].reshape(main, half),
            lambda: early_in[j, :, :, :half].reshape(main, half),
            j,
        )
        late_made[j, :, :, :half] = late_value.reshape(chunks, MAIN, half)
        write(late_made.at[j, :, :, body], late_out[j].at[:, :, body])
        early_made[j, :, :, :half] = early_value.reshape(chunks, MAIN, half)
        write(early_made.at[j, :, :, body], early_out.at[:, j, :, body])

    matrix = split_matrix()

    def gather_last(buffer):
        return pieces_to_rows(buffer[:, :, :, half:].reshape(RING * main, width - half), matrix)

    late_rows, early_rows = gather_last(late_in), gather_last(early_in)
    late_value, early_value = half_expert(lambda: late_rows, lambda: early_rows)
    for value, made in ((late_value, late_made), (early_value, early_made)):
        for j in range(RING):
            pieces = rows_to_pieces(value[last * j : last * (j + 1)], matrix)
            made[j, :, :, half:] = pieces.reshape(chunks, MAIN, width - half)
    for j in range(RING):
        write(late_made.at[j, :, :, tail], late_out[j].at[:, :, tail])
        write(early_made.at[j, :, :, tail], early_out.at[:, j, :, tail])
    for copy in writes:
        copy.wait()


def half_ffn(late, early, w_gate, w_up, w_down):
    chunks, _, width = late[0].shape
    model, hidden = w_gate.shape[1:]
    rows = RING * chunks * CAP
    outside = pl.BlockSpec(memory_space=pltpu.HBM)
    buffer = pltpu.VMEM((RING, chunks, MAIN, width), jnp.bfloat16)
    late_shape = jax.ShapeDtypeStruct(late[0].shape, jnp.bfloat16)
    *late_out, early_out = pl.pallas_call(
        ffn_kernel,
        in_specs=[outside] * (RING + 4),
        out_specs=[outside] * (RING + 1),
        out_shape=[late_shape] * RING + [jax.ShapeDtypeStruct(early.shape, jnp.bfloat16)],
        scratch_shapes=[
            buffer,
            buffer,
            pltpu.VMEM((model, hidden), jnp.bfloat16),
            pltpu.VMEM((model, hidden), jnp.bfloat16),
            pltpu.VMEM((hidden, model), jnp.bfloat16),
            buffer,
            buffer,
            pltpu.SemaphoreType.DMA((2 * RING + 5,)),
            pltpu.SemaphoreType.DMA((4 * RING,)),
        ],
        cost_estimate=pl.CostEstimate(
            flops=6 * rows * model * hidden,
            bytes_accessed=4 * rows * model + 6 * model * hidden,
            transcendentals=rows * hidden,
        ),
        compiler_params=pltpu.CompilerParams(vmem_limit_bytes=56 * 1024 * 1024),
        name="half_ffn",
    )(*late, early, w_gate, w_up, w_down)
    return late_out, early_out


def sum_halves_kernel(a_ref, b_ref, c_ref, d_ref, out_ref):
    for r, (first, second) in enumerate(((a_ref, b_ref), (c_ref, d_ref))):
        for i in range(0, first.shape[0], 8):
            both = first[i : i + 8].astype(jnp.float32) + second[i : i + 8].astype(jnp.float32)
            out_ref[i : i + 8, r] = both.astype(jnp.bfloat16)


def sum_halves(arrays):
    chunks, _, width = arrays[0].shape
    on_chip = pl.BlockSpec(memory_space=pltpu.VMEM)
    return pl.pallas_call(
        sum_halves_kernel,
        in_specs=[on_chip] * RING,
        out_specs=on_chip,
        out_shape=jax.ShapeDtypeStruct((chunks, 2, MAIN, width), jnp.bfloat16),
        cost_estimate=pl.CostEstimate(
            flops=4 * chunks * MAIN * width, bytes_accessed=12 * chunks * MAIN * width,
            transcendentals=0,
        ),
        compiler_params=pltpu.CompilerParams(vmem_limit_bytes=12 * 1024 * 1024),
        name="sum_halves",
    )(*arrays)


def early_combine_kernel(pair_ref, ids_ref, gates_ref, rows_ref, out_ref):
    chunks = rows_ref.shape[0]
    _, count, half = out_ref.shape
    expert = own_pair(chunks, count, pair_ref[0])
    slot, weight = slots_of(ids_ref[0], expert, gates_ref[0])
    main = rows_ref[:, 0, :, :half].reshape(chunks * MAIN, half)
    pieces = rows_ref[:, 0, :, half:].reshape(chunks * MAIN, half // PIECES)
    out_ref[0] = combine_rows(slot, weight, main, pieces).astype(jnp.bfloat16)


def early_combine(pair, ids_t, gates_t, rows):
    chunks, ring, _, width = rows.shape
    count = ids_t.shape[2]
    half = width * MAIN // CAP
    return pl.pallas_call(
        early_combine_kernel,
        grid=(ring,),
        in_specs=[
            pl.BlockSpec(memory_space=pltpu.SMEM),
            pl.BlockSpec((1,) + ids_t.shape[1:], lambda i: (i, 0, 0)),
            pl.BlockSpec((1,) + gates_t.shape[1:], lambda i: (i, 0, 0)),
            pl.BlockSpec((chunks, 1, MAIN, width), lambda i: (0, i, 0, 0)),
        ],
        out_specs=pl.BlockSpec((1, count, half), lambda i: (i, 0, 0)),
        out_shape=jax.ShapeDtypeStruct((ring, count, half), jnp.bfloat16),
        cost_estimate=pl.CostEstimate(
            flops=2 * ring * chunks * CAP * count * half,
            bytes_accessed=2 * ring * chunks * MAIN * width,
            transcendentals=0,
        ),
        compiler_params=pltpu.CompilerParams(vmem_limit_bytes=12 * 1024 * 1024),
        name="early_combine",
    )(pair, ids_t, gates_t, rows)


def final_kernel(pair_ref, ids_ref, gates_ref, rows_ref, *refs):
    parts, (out_ref, slot_ref, weight_ref) = refs[:RING], refs[RING:]
    experts = rows_ref.shape[0]
    half = parts[0].shape[1]
    block = 16
    expert = near_first(*slot_ref.shape, pair_ref[0])
    slot, weight = slots_of(ids_ref[...], expert, gates_ref[...])
    slot_ref[...] = slot
    weight_ref[...] = weight
    total = jnp.zeros((slot.shape[1], half), jnp.float32)
    for first in range(0, experts, block):
        here = slice(first, first + block)
        main = rows_ref[here, :, :half].reshape(block * MAIN, half)
        pieces = rows_ref[here, :, half:].reshape(block * MAIN, half // PIECES)
        total += combine_rows(slot_ref[here, :], weight_ref[here, :], main, pieces)
    out_ref[:, :half] = total.astype(jnp.bfloat16)
    total = parts[0][...].astype(jnp.float32)
    for part in parts[1:]:
        total += part[...].astype(jnp.float32)
    out_ref[:, half:] = total.astype(jnp.bfloat16)


def final_combine(pair, ids_t, gates_t, rows, parts):
    experts, _, width = rows.shape
    count, half = parts[0].shape
    on_chip = pl.BlockSpec(memory_space=pltpu.VMEM)
    return pl.pallas_call(
        final_kernel,
        in_specs=[pl.BlockSpec(memory_space=pltpu.SMEM)] + [on_chip] * (3 + RING),
        out_specs=on_chip,
        out_shape=jax.ShapeDtypeStruct((count, 2 * half), jnp.bfloat16),
        scratch_shapes=[
            pltpu.VMEM((experts, count), jnp.float32),
            pltpu.VMEM((experts, count), jnp.float32),
        ],
        cost_estimate=pl.CostEstimate(
            flops=2 * experts * CAP * count * half,
            bytes_accessed=2 * experts * MAIN * width,
            transcendentals=0,
        ),
        compiler_params=pltpu.CompilerParams(vmem_limit_bytes=16 * 1024 * 1024),
        name="final_combine",
    )(pair, ids_t, gates_t, rows, *parts)


def across(array, j):
    return lax.ppermute(array, "y", [(y, y ^ j) for y in range(RING)])


def gather_ring(array):
    return jnp.stack([array] + [across(array, j) for j in range(1, RING)])


def plane_exchange(array):
    return lax.all_to_all(array, PLANE, split_axis=0, concat_axis=0, tiled=True)


def per_device(tokens, expert_ids, gate_weights, w_gate, w_up, w_down):
    chunks = lax.axis_size("grp") * lax.axis_size("x")
    experts = 2 * chunks
    top = expert_ids.shape[1]
    half = tokens.shape[1] // 2
    pair = (lax.axis_index("y") // 2).astype(jnp.int32).reshape(1)
    ids_t = expert_ids.T
    gates_t = gate_weights.T

    late = late_dispatch(pair, ids_t, tokens, experts)
    width = late.shape[2]
    late = plane_exchange(late.reshape(chunks, 2 * MAIN, width))
    late = late.reshape(chunks, 2, MAIN, width)
    near, far = late[:, 0], late[:, 1]

    routing = gather_ring(jnp.concatenate([ids_t.astype(jnp.bfloat16), gates_t], axis=0))
    ids_ring = routing[:, :top].astype(jnp.int32)
    gates_ring = routing[:, top:].astype(jnp.float32)
    early = early_dispatch(pair, ids_ring, gather_ring(tokens[:, half:]), chunks)
    early = plane_exchange(early.reshape(chunks, RING * MAIN, width))
    early = early.reshape(chunks, RING, MAIN, width)

    late_in = (near, across(near, 1), across(far, 2), across(far, 3))
    late_out, early_out = half_ffn(late_in, early, w_gate, w_up, w_down)
    late_back = [late_out[0]]
    for j in range(1, RING):
        late_back.append(across(late_out[j], j))
    early_out = plane_exchange(early_out.reshape(chunks, RING * MAIN, width))
    late_back = plane_exchange(sum_halves(late_back).reshape(chunks, 2 * MAIN, width))
    partial = early_combine(
        pair, ids_ring, gates_ring, early_out.reshape(chunks, RING, MAIN, width)
    )
    parts = [partial[0]] + [across(partial[j], j) for j in range(1, RING)]
    return final_combine(
        pair, ids_t, gates_t.astype(jnp.float32), late_back.reshape(experts, MAIN, width), parts
    )


def solution(mesh):
    ring = Mesh(mesh.devices.reshape(mesh.devices.shape[0], -1, RING), AXES)
    rows = P(AXES, None)
    weights = P(AXES, None, None)

    return jax.shard_map(
        per_device,
        mesh=ring,
        in_specs=(rows, rows, rows, weights, weights, weights),
        out_specs=rows,
        check_vma=False,
    )
```

```python
import jax
import jax.numpy as jnp
from jax import lax
from jax.experimental import pallas as pl
from jax.experimental.pallas import tpu as pltpu
from jax.sharding import Mesh, PartitionSpec as P

AXES = ("grp", "x", "y")
PLANE = ("grp", "x")
CAP = 18
MAIN = 16
PIECES = 8
TILE = MAIN * PIECES
RING = 4
BATCHES = ((0, 1), (3, 2))


def split_matrix():
    row = lax.broadcasted_iota(jnp.int32, (TILE, TILE), 0)
    col = lax.broadcasted_iota(jnp.int32, (TILE, TILE), 1)
    source = (row % MAIN) // 2 * MAIN + (row % 2) * PIECES + row // MAIN
    return (source == col).astype(jnp.bfloat16)


def exact_dot(a, b, dims=((1,), (0,))):
    return lax.dot_general(a, b, (dims, ((), ())), preferred_element_type=jnp.float32)


def pieces_to_rows(pieces, matrix):
    tiles = []
    for tile in range(pieces.shape[0] // TILE):
        stacked = exact_dot(matrix, pieces[TILE * tile : TILE * (tile + 1)])
        stacked = stacked.astype(jnp.bfloat16)
        tiles.append(
            jnp.concatenate([stacked[MAIN * q : MAIN * (q + 1)] for q in range(PIECES)], axis=1)
        )
    return jnp.concatenate(tiles, axis=0)


def rows_to_pieces(rows, matrix):
    width = rows.shape[1] // PIECES
    tiles = []
    for tile in range(rows.shape[0] // MAIN):
        part = rows[MAIN * tile : MAIN * (tile + 1)]
        stacked = jnp.concatenate(
            [part[:, width * q : width * (q + 1)] for q in range(PIECES)], axis=0
        )
        tiles.append(exact_dot(matrix, stacked, ((0,), (0,))).astype(jnp.bfloat16))
    return jnp.concatenate(tiles, axis=0)


def slots_of(ids_t, expert, gates_t=None):
    count = ids_t.shape[1]
    used = jnp.zeros(expert.shape, jnp.float32)
    weight = jnp.zeros(expert.shape, jnp.float32)
    for k in range(ids_t.shape[0]):
        hit = expert == ids_t[k : k + 1, :]
        used = jnp.where(hit, 1.0, used)
        if gates_t is not None:
            weight = jnp.where(hit, gates_t[k : k + 1, :], weight)
    earlier = lax.broadcasted_iota(jnp.int32, (count, count), 0)
    later = lax.broadcasted_iota(jnp.int32, (count, count), 1)
    before = exact_dot(used.astype(jnp.bfloat16), (earlier < later).astype(jnp.bfloat16))
    return jnp.where(used > 0.0, before, -1.0), weight


def near_first(rows, count, pair):
    row = lax.broadcasted_iota(jnp.int32, (rows, count), 0)
    other = row % 2
    return row - other + jnp.where(other == 0, pair, 1 - pair)


def own_pair(rows, count, pair):
    return 2 * lax.broadcasted_iota(jnp.int32, (rows, count), 0) + pair


def pick_rows(slot, tokens):
    block, count = slot.shape
    model = tokens.shape[1]
    main_id = lax.broadcasted_iota(jnp.int32, (block, MAIN, count), 1).astype(jnp.float32)
    pick = (slot[:, None, :] == main_id).astype(jnp.float32).reshape(block * MAIN, count)
    rows = exact_dot(pick.astype(jnp.bfloat16), tokens).astype(jnp.bfloat16)
    row = lax.broadcasted_iota(jnp.int32, (2 * block, count), 0)
    slot_twice = jnp.broadcast_to(slot[:, None, :], (block, 2, count)).reshape(2 * block, count)
    pick_last = (slot_twice == (MAIN + row % 2).astype(jnp.float32)).astype(jnp.bfloat16)
    last = exact_dot(pick_last, tokens).astype(jnp.bfloat16)
    pieces = rows_to_pieces(last, split_matrix())
    return rows.reshape(block, MAIN, model), pieces.reshape(block, MAIN, model // PIECES)


def combine_rows(slot, weight, main, pieces):
    block, count = slot.shape

    def spread(first, slots):
        shape = (block, slots, count)
        slot_id = first + lax.broadcasted_iota(jnp.int32, shape, 1)
        hit = slot[:, None, :] == slot_id.astype(jnp.float32)
        scaled = jnp.where(hit, jnp.broadcast_to(weight[:, None, :], shape), 0.0)
        return scaled.reshape(block * slots, count).astype(jnp.bfloat16)

    total = exact_dot(spread(0, MAIN), main, ((0,), (0,)))
    last = pieces_to_rows(pieces, split_matrix())
    return total + exact_dot(spread(MAIN, CAP - MAIN), last, ((0,), (0,)))


def late_dispatch_kernel(pair_ref, ids_ref, tokens_ref, out_ref, slot_ref):
    block, _, _ = out_ref.shape
    model = tokens_ref.shape[1]
    step = pl.program_id(0)

    @pl.when(step == 0)
    def _():
        expert = near_first(*slot_ref.shape, pair_ref[0])
        slot_ref[...] = slots_of(ids_ref[...], expert)[0]

    slot = slot_ref[pl.ds(pl.multiple_of(step * block, block), block), :]
    rows, pieces = pick_rows(slot, tokens_ref[...])
    out_ref[:, :, :model] = rows
    out_ref[:, :, model:] = pieces


def late_dispatch(pair, ids_t, tokens, experts):
    count, model = tokens.shape
    half = model // 2
    width = half * CAP // MAIN
    block = 16
    return pl.pallas_call(
        late_dispatch_kernel,
        grid=(experts // block,),
        in_specs=[
            pl.BlockSpec(memory_space=pltpu.SMEM),
            pl.BlockSpec(ids_t.shape, lambda i: (0, 0)),
            pl.BlockSpec((count, half), lambda i: (0, 0)),
        ],
        out_specs=pl.BlockSpec((block, MAIN, width), lambda i: (i, 0, 0)),
        out_shape=jax.ShapeDtypeStruct((experts, MAIN, width), jnp.bfloat16),
        scratch_shapes=[pltpu.VMEM((experts, count), jnp.float32)],
        cost_estimate=pl.CostEstimate(
            flops=2 * experts * CAP * count * half,
            bytes_accessed=2 * experts * MAIN * width,
            transcendentals=0,
        ),
        name="late_dispatch",
    )(pair, ids_t, tokens)


def early_dispatch_kernel(pair_ref, ids_ref, tokens_ref, out_ref):
    chunks = out_ref.shape[0]
    _, count, model = tokens_ref.shape
    expert = own_pair(chunks, count, pair_ref[0])
    slot = slots_of(ids_ref[0], expert)[0]
    rows, pieces = pick_rows(slot, tokens_ref[0])
    out_ref[:, 0, :, :model] = rows
    out_ref[:, 0, :, model:] = pieces


def early_dispatch(pair, ids_t, tokens, chunks):
    ring, count, half = tokens.shape
    width = half * CAP // MAIN
    return pl.pallas_call(
        early_dispatch_kernel,
        grid=(ring,),
        in_specs=[
            pl.BlockSpec(memory_space=pltpu.SMEM),
            pl.BlockSpec((1,) + ids_t.shape[1:], lambda i: (i, 0, 0)),
            pl.BlockSpec((1, count, half), lambda i: (i, 0, 0)),
        ],
        out_specs=pl.BlockSpec((chunks, 1, MAIN, width), lambda i: (0, i, 0, 0)),
        out_shape=jax.ShapeDtypeStruct((chunks, ring, MAIN, width), jnp.bfloat16),
        cost_estimate=pl.CostEstimate(
            flops=2 * ring * chunks * CAP * count * half,
            bytes_accessed=2 * ring * chunks * MAIN * width,
            transcendentals=0,
        ),
        name="early_dispatch",
    )(pair, ids_t, tokens)


def ffn_kernel(*refs):
    late_in, early_in, gate_w, up_w, down_w, late_made, early_made, in_sems, out_sems = refs[-9:]
    places, chunks, _, width = late_in.shape
    late_hbm, late_out, early_out = refs[:places], refs[places + 4 : -10], refs[-10]
    early_hbm, gate_hbm, up_hbm, down_hbm = refs[places : places + 4]
    model = gate_w.shape[1]
    half = model // 2
    main = chunks * MAIN
    last = 2 * chunks
    first, second = pl.ds(0, half), pl.ds(half, half)
    body, tail = pl.ds(0, half), pl.ds(half, width - half)

    reads = {}

    def read(name, source, target):
        reads[name] = pltpu.make_async_copy(source, target, in_sems.at[len(reads)])
        reads[name].start()

    def read_rows(j):
        read(("late", j), late_hbm[j], late_in.at[j])
        read(("early", j), early_hbm.at[:, j], early_in.at[j])

    read("gate_first", gate_hbm.at[0, :, first], gate_w.at[:, first])
    read(("late", 0), late_hbm[0], late_in.at[0])
    read("up_first", up_hbm.at[0, :, first], up_w.at[:, first])
    read(("early", 0), early_hbm.at[:, 0], early_in.at[0])
    read("gate_second", gate_hbm.at[0, :, second], gate_w.at[:, second])
    read("up_second", up_hbm.at[0, :, second], up_w.at[:, second])
    read("down", down_hbm.at[0], down_w)
    for j in range(1, places):
        read_rows(j)

    waited = set()

    def ready(*names):
        for name in names:
            if name not in waited:
                waited.add(name)
                reads[name].wait()

    writes = []

    def write(source, target):
        writes.append(pltpu.make_async_copy(source, target, out_sems.at[len(writes)]))
        writes[-1].start()

    def half_expert(late, early, j=None):
        if j is not None:
            ready("gate_first", ("late", j))
        gate = exact_dot(late(), gate_w[:, :half], ((1,), (1,)))
        ready("up_first")
        up = exact_dot(late(), up_w[:, :half], ((1,), (1,)))
        if j is not None:
            ready(("early", j), "gate_second")
        gate = gate + exact_dot(early(), gate_w[:, half:], ((1,), (1,)))
        ready("up_second")
        up = up + exact_dot(early(), up_w[:, half:], ((1,), (1,)))
        hidden = (gate / (1.0 + jnp.exp(-gate)) * up).astype(jnp.bfloat16)
        ready("down")
        late_value = exact_dot(hidden, down_w[:, :half]).astype(jnp.bfloat16)
        early_value = exact_dot(hidden, down_w[:, half:]).astype(jnp.bfloat16)
        return late_value, early_value

    for j in range(places):
        late_value, early_value = half_expert(
            lambda: late_in[j, :, :, :half].reshape(main, half),
            lambda: early_in[j, :, :, :half].reshape(main, half),
            j,
        )
        late_made[j, :, :, :half] = late_value.reshape(chunks, MAIN, half)
        write(late_made.at[j, :, :, body], late_out[j].at[:, :, body])
        early_made[j, :, :, :half] = early_value.reshape(chunks, MAIN, half)
        write(early_made.at[j, :, :, body], early_out.at[:, j, :, body])

    matrix = split_matrix()

    def gather_last(buffer):
        return pieces_to_rows(buffer[:, :, :, half:].reshape(places * main, width - half), matrix)

    late_rows, early_rows = gather_last(late_in), gather_last(early_in)
    late_value, early_value = half_expert(lambda: late_rows, lambda: early_rows)
    for value, made in ((late_value, late_made), (early_value, early_made)):
        for j in range(places):
            pieces = rows_to_pieces(value[last * j : last * (j + 1)], matrix)
            made[j, :, :, half:] = pieces.reshape(chunks, MAIN, width - half)
    for j in range(places):
        write(late_made.at[j, :, :, tail], late_out[j].at[:, :, tail])
        write(early_made.at[j, :, :, tail], early_out.at[:, j, :, tail])
    for copy in writes:
        copy.wait()


def half_ffn(late, early, w_gate, w_up, w_down):
    places = len(late)
    chunks, _, width = late[0].shape
    model, hidden = w_gate.shape[1:]
    rows = places * chunks * CAP
    outside = pl.BlockSpec(memory_space=pltpu.HBM)
    buffer = pltpu.VMEM((places, chunks, MAIN, width), jnp.bfloat16)
    late_shape = jax.ShapeDtypeStruct(late[0].shape, jnp.bfloat16)
    *late_out, early_out = pl.pallas_call(
        ffn_kernel,
        in_specs=[outside] * (places + 4),
        out_specs=[outside] * (places + 1),
        out_shape=[late_shape] * places + [jax.ShapeDtypeStruct(early.shape, jnp.bfloat16)],
        scratch_shapes=[
            buffer,
            buffer,
            pltpu.VMEM((hidden, model), jnp.bfloat16),
            pltpu.VMEM((hidden, model), jnp.bfloat16),
            pltpu.VMEM((hidden, model), jnp.bfloat16),
            buffer,
            buffer,
            pltpu.SemaphoreType.DMA((2 * places + 5,)),
            pltpu.SemaphoreType.DMA((4 * places,)),
        ],
        cost_estimate=pl.CostEstimate(
            flops=6 * rows * model * hidden,
            bytes_accessed=4 * rows * model + 6 * model * hidden,
            transcendentals=rows * hidden,
        ),
        compiler_params=pltpu.CompilerParams(vmem_limit_bytes=56 * 1024 * 1024),
        name="half_ffn",
    )(*late, early, w_gate.swapaxes(1, 2), w_up.swapaxes(1, 2), w_down)
    return late_out, early_out


def sum_halves_kernel(a_ref, b_ref, c_ref, d_ref, out_ref):
    for r, (first, second) in enumerate(((a_ref, b_ref), (c_ref, d_ref))):
        for i in range(0, first.shape[0], 8):
            both = first[i : i + 8].astype(jnp.float32) + second[i : i + 8].astype(jnp.float32)
            out_ref[i : i + 8, r] = both.astype(jnp.bfloat16)


def sum_halves(arrays):
    chunks, _, width = arrays[0].shape
    on_chip = pl.BlockSpec(memory_space=pltpu.VMEM)
    return pl.pallas_call(
        sum_halves_kernel,
        in_specs=[on_chip] * RING,
        out_specs=on_chip,
        out_shape=jax.ShapeDtypeStruct((chunks, 2, MAIN, width), jnp.bfloat16),
        cost_estimate=pl.CostEstimate(
            flops=4 * chunks * MAIN * width, bytes_accessed=12 * chunks * MAIN * width,
            transcendentals=0,
        ),
        compiler_params=pltpu.CompilerParams(vmem_limit_bytes=12 * 1024 * 1024),
        name="sum_halves",
    )(*arrays)


def early_combine_kernel(pair_ref, ids_ref, gates_ref, rows_ref, out_ref):
    chunks = rows_ref.shape[0]
    _, count, half = out_ref.shape
    expert = own_pair(chunks, count, pair_ref[0])
    slot, weight = slots_of(ids_ref[0], expert, gates_ref[0])
    main = rows_ref[:, 0, :, :half].reshape(chunks * MAIN, half)
    pieces = rows_ref[:, 0, :, half:].reshape(chunks * MAIN, half // PIECES)
    out_ref[0] = combine_rows(slot, weight, main, pieces).astype(jnp.bfloat16)


def early_combine(pair, ids_t, gates_t, rows):
    chunks, ring, _, width = rows.shape
    count = ids_t.shape[2]
    half = width * MAIN // CAP
    return pl.pallas_call(
        early_combine_kernel,
        grid=(ring,),
        in_specs=[
            pl.BlockSpec(memory_space=pltpu.SMEM),
            pl.BlockSpec((1,) + ids_t.shape[1:], lambda i: (i, 0, 0)),
            pl.BlockSpec((1,) + gates_t.shape[1:], lambda i: (i, 0, 0)),
            pl.BlockSpec((chunks, 1, MAIN, width), lambda i: (0, i, 0, 0)),
        ],
        out_specs=pl.BlockSpec((1, count, half), lambda i: (i, 0, 0)),
        out_shape=jax.ShapeDtypeStruct((ring, count, half), jnp.bfloat16),
        cost_estimate=pl.CostEstimate(
            flops=2 * ring * chunks * CAP * count * half,
            bytes_accessed=2 * ring * chunks * MAIN * width,
            transcendentals=0,
        ),
        compiler_params=pltpu.CompilerParams(vmem_limit_bytes=12 * 1024 * 1024),
        name="early_combine",
    )(pair, ids_t, gates_t, rows)


def final_kernel(pair_ref, ids_ref, gates_ref, rows_ref, *refs):
    parts, (out_ref, slot_ref, weight_ref) = refs[:RING], refs[RING:]
    experts = rows_ref.shape[0]
    half = parts[0].shape[1]
    block = 16
    expert = near_first(*slot_ref.shape, pair_ref[0])
    slot, weight = slots_of(ids_ref[...], expert, gates_ref[...])
    slot_ref[...] = slot
    weight_ref[...] = weight
    total = jnp.zeros((slot.shape[1], half), jnp.float32)
    for first in range(0, experts, block):
        here = slice(first, first + block)
        main = rows_ref[here, :, :half].reshape(block * MAIN, half)
        pieces = rows_ref[here, :, half:].reshape(block * MAIN, half // PIECES)
        total += combine_rows(slot_ref[here, :], weight_ref[here, :], main, pieces)
    out_ref[:, :half] = total.astype(jnp.bfloat16)
    total = parts[0][...].astype(jnp.float32)
    for part in parts[1:]:
        total += part[...].astype(jnp.float32)
    out_ref[:, half:] = total.astype(jnp.bfloat16)


def final_combine(pair, ids_t, gates_t, rows, parts):
    experts, _, width = rows.shape
    count, half = parts[0].shape
    on_chip = pl.BlockSpec(memory_space=pltpu.VMEM)
    return pl.pallas_call(
        final_kernel,
        in_specs=[pl.BlockSpec(memory_space=pltpu.SMEM)] + [on_chip] * (3 + RING),
        out_specs=on_chip,
        out_shape=jax.ShapeDtypeStruct((count, 2 * half), jnp.bfloat16),
        scratch_shapes=[
            pltpu.VMEM((experts, count), jnp.float32),
            pltpu.VMEM((experts, count), jnp.float32),
        ],
        cost_estimate=pl.CostEstimate(
            flops=2 * experts * CAP * count * half,
            bytes_accessed=2 * experts * MAIN * width,
            transcendentals=0,
        ),
        compiler_params=pltpu.CompilerParams(vmem_limit_bytes=16 * 1024 * 1024),
        name="final_combine",
    )(pair, ids_t, gates_t, rows, *parts)


def across(array, j):
    return lax.ppermute(array, "y", [(y, y ^ j) for y in range(RING)])


def at_places(array):
    arrays = [array]
    for j in range(1, RING):
        arrays.append(across(array, j))
    return arrays


def plane_exchange(array):
    return lax.all_to_all(array, PLANE, split_axis=0, concat_axis=0, tiled=True)


def per_device(tokens, expert_ids, gate_weights, w_gate, w_up, w_down):
    chunks = lax.axis_size("grp") * lax.axis_size("x")
    experts = 2 * chunks
    top = expert_ids.shape[1]
    half = tokens.shape[1] // 2
    pair = (lax.axis_index("y") // 2).astype(jnp.int32).reshape(1)
    ids_t = expert_ids.T
    gates_t = gate_weights.T

    late = late_dispatch(pair, ids_t, tokens, experts)
    width = late.shape[2]
    late = plane_exchange(late.reshape(chunks, 2 * MAIN, width))
    late = late.reshape(chunks, 2, MAIN, width)
    near, far = late[:, 0], late[:, 1]

    routing = at_places(jnp.concatenate([ids_t.astype(jnp.bfloat16), gates_t], axis=0))
    tokens_at = at_places(tokens[:, half:])
    late_in = [near]
    for j in range(1, RING):
        late_in.append(across(near if j == 1 else far, j))
    late_back, parts = [None] * RING, [None] * RING
    arrived, ids_ring, gates_ring = [], [], []
    for batch, places in enumerate(BATCHES):
        table = jnp.stack([routing[j] for j in places])
        ids_ring.append(table[:, :top].astype(jnp.int32))
        gates_ring.append(table[:, top:].astype(jnp.float32))
        tokens_here = jnp.stack([tokens_at[j] for j in places])
        early = early_dispatch(pair, ids_ring[batch], tokens_here, chunks)
        early = plane_exchange(early.reshape(chunks, len(places) * MAIN, width))
        arrived.append(early.reshape(chunks, len(places), MAIN, width))

    early_back = []
    for batch, places in enumerate(BATCHES):
        late_out, early_out = half_ffn(
            [late_in[j] for j in places], arrived[batch], w_gate, w_up, w_down
        )
        for j, rows in zip(places, late_out):
            late_back[j] = across(rows, j) if j else rows
        early_back.append(plane_exchange(early_out.reshape(chunks, -1, width)))

    late_back = plane_exchange(sum_halves(late_back).reshape(chunks, 2 * MAIN, width))
    for batch, places in enumerate(BATCHES):
        rows = early_back[batch].reshape(chunks, len(places), MAIN, width)
        partial = early_combine(pair, ids_ring[batch], gates_ring[batch], rows)
        for i, j in enumerate(places):
            parts[j] = across(partial[i], j) if j else partial[i]
    return final_combine(
        pair, ids_t, gates_t.astype(jnp.float32), late_back.reshape(experts, MAIN, width), parts
    )


def solution(mesh):
    ring = Mesh(mesh.devices.reshape(mesh.devices.shape[0], -1, RING), AXES)
    rows = P(AXES, None)
    weights = P(AXES, None, None)

    return jax.shard_map(
        per_device,
        mesh=ring,
        in_specs=(rows, rows, rows, weights, weights, weights),
        out_specs=rows,
        check_vma=False,
    )
```

```python
import jax
import jax.numpy as jnp
from jax import lax
from jax.experimental import pallas as pl
from jax.experimental.pallas import tpu as pltpu
from jax.sharding import Mesh, PartitionSpec as P

AXES = ("grp", "x", "y")
PLANE = ("grp", "x")
CAP = 18
MAIN = 16
PIECES = 8
TILE = MAIN * PIECES
RING = 4
BATCHES = ((1, 3), (0, 2))


def split_matrix():
    row = lax.broadcasted_iota(jnp.int32, (TILE, TILE), 0)
    col = lax.broadcasted_iota(jnp.int32, (TILE, TILE), 1)
    source = (row % MAIN) // 2 * MAIN + (row % 2) * PIECES + row // MAIN
    return (source == col).astype(jnp.bfloat16)


def exact_dot(a, b, dims=((1,), (0,))):
    return lax.dot_general(a, b, (dims, ((), ())), preferred_element_type=jnp.float32)


def pieces_to_rows(pieces, matrix):
    tiles = []
    for tile in range(pieces.shape[0] // TILE):
        stacked = exact_dot(matrix, pieces[TILE * tile : TILE * (tile + 1)])
        stacked = stacked.astype(jnp.bfloat16)
        tiles.append(
            jnp.concatenate([stacked[MAIN * q : MAIN * (q + 1)] for q in range(PIECES)], axis=1)
        )
    return jnp.concatenate(tiles, axis=0)


def rows_to_pieces(rows, matrix):
    width = rows.shape[1] // PIECES
    tiles = []
    for tile in range(rows.shape[0] // MAIN):
        part = rows[MAIN * tile : MAIN * (tile + 1)]
        stacked = jnp.concatenate(
            [part[:, width * q : width * (q + 1)] for q in range(PIECES)], axis=0
        )
        tiles.append(exact_dot(matrix, stacked, ((0,), (0,))).astype(jnp.bfloat16))
    return jnp.concatenate(tiles, axis=0)


def slots_of(ids_t, expert, gates_t=None):
    count = ids_t.shape[1]
    used = jnp.zeros(expert.shape, jnp.float32)
    weight = jnp.zeros(expert.shape, jnp.float32)
    for k in range(ids_t.shape[0]):
        hit = expert == ids_t[k : k + 1, :]
        used = jnp.where(hit, 1.0, used)
        if gates_t is not None:
            weight = jnp.where(hit, gates_t[k : k + 1, :], weight)
    earlier = lax.broadcasted_iota(jnp.int32, (count, count), 0)
    later = lax.broadcasted_iota(jnp.int32, (count, count), 1)
    before = exact_dot(used.astype(jnp.bfloat16), (earlier < later).astype(jnp.bfloat16))
    return jnp.where(used > 0.0, before, -1.0), weight


def near_first(rows, count, pair):
    row = lax.broadcasted_iota(jnp.int32, (rows, count), 0)
    other = row % 2
    return row - other + jnp.where(other == 0, pair, 1 - pair)


def own_pair(rows, count, pair):
    return 2 * lax.broadcasted_iota(jnp.int32, (rows, count), 0) + pair


def pick_rows(slot, tokens):
    block, count = slot.shape
    model = tokens.shape[1]
    main_id = lax.broadcasted_iota(jnp.int32, (block, MAIN, count), 1).astype(jnp.float32)
    pick = (slot[:, None, :] == main_id).astype(jnp.float32).reshape(block * MAIN, count)
    rows = exact_dot(pick.astype(jnp.bfloat16), tokens).astype(jnp.bfloat16)
    row = lax.broadcasted_iota(jnp.int32, (2 * block, count), 0)
    slot_twice = jnp.broadcast_to(slot[:, None, :], (block, 2, count)).reshape(2 * block, count)
    pick_last = (slot_twice == (MAIN + row % 2).astype(jnp.float32)).astype(jnp.bfloat16)
    last = exact_dot(pick_last, tokens).astype(jnp.bfloat16)
    pieces = rows_to_pieces(last, split_matrix())
    return rows.reshape(block, MAIN, model), pieces.reshape(block, MAIN, model // PIECES)


def combine_rows(slot, weight, main, pieces):
    block, count = slot.shape

    def spread(first, slots):
        shape = (block, slots, count)
        slot_id = first + lax.broadcasted_iota(jnp.int32, shape, 1)
        hit = slot[:, None, :] == slot_id.astype(jnp.float32)
        scaled = jnp.where(hit, jnp.broadcast_to(weight[:, None, :], shape), 0.0)
        return scaled.reshape(block * slots, count).astype(jnp.bfloat16)

    total = exact_dot(spread(0, MAIN), main, ((0,), (0,)))
    last = pieces_to_rows(pieces, split_matrix())
    return total + exact_dot(spread(MAIN, CAP - MAIN), last, ((0,), (0,)))


def late_dispatch_kernel(pair_ref, ids_ref, tokens_ref, out_ref, slot_ref):
    block, _, _ = out_ref.shape
    model = tokens_ref.shape[1]
    step = pl.program_id(0)

    @pl.when(step == 0)
    def _():
        expert = near_first(*slot_ref.shape, pair_ref[0])
        slot_ref[...] = slots_of(ids_ref[...], expert)[0]

    slot = slot_ref[pl.ds(pl.multiple_of(step * block, block), block), :]
    rows, pieces = pick_rows(slot, tokens_ref[...])
    out_ref[:, :, :model] = rows
    out_ref[:, :, model:] = pieces


def late_dispatch(pair, ids_t, tokens, experts):
    count, model = tokens.shape
    half = model // 2
    width = half * CAP // MAIN
    block = 16
    return pl.pallas_call(
        late_dispatch_kernel,
        grid=(experts // block,),
        in_specs=[
            pl.BlockSpec(memory_space=pltpu.SMEM),
            pl.BlockSpec(ids_t.shape, lambda i: (0, 0)),
            pl.BlockSpec((count, half), lambda i: (0, 0)),
        ],
        out_specs=pl.BlockSpec((block, MAIN, width), lambda i: (i, 0, 0)),
        out_shape=jax.ShapeDtypeStruct((experts, MAIN, width), jnp.bfloat16),
        scratch_shapes=[pltpu.VMEM((experts, count), jnp.float32)],
        cost_estimate=pl.CostEstimate(
            flops=2 * experts * CAP * count * half,
            bytes_accessed=2 * experts * MAIN * width,
            transcendentals=0,
        ),
        name="late_dispatch",
    )(pair, ids_t, tokens)


def early_dispatch_kernel(pair_ref, ids_ref, tokens_ref, out_ref):
    chunks = out_ref.shape[0]
    _, count, model = tokens_ref.shape
    expert = own_pair(chunks, count, pair_ref[0])
    slot = slots_of(ids_ref[0], expert)[0]
    rows, pieces = pick_rows(slot, tokens_ref[0])
    out_ref[:, 0, :, :model] = rows
    out_ref[:, 0, :, model:] = pieces


def early_dispatch(pair, ids_t, tokens, chunks):
    ring, count, half = tokens.shape
    width = half * CAP // MAIN
    return pl.pallas_call(
        early_dispatch_kernel,
        grid=(ring,),
        in_specs=[
            pl.BlockSpec(memory_space=pltpu.SMEM),
            pl.BlockSpec((1,) + ids_t.shape[1:], lambda i: (i, 0, 0)),
            pl.BlockSpec((1, count, half), lambda i: (i, 0, 0)),
        ],
        out_specs=pl.BlockSpec((chunks, 1, MAIN, width), lambda i: (0, i, 0, 0)),
        out_shape=jax.ShapeDtypeStruct((chunks, ring, MAIN, width), jnp.bfloat16),
        cost_estimate=pl.CostEstimate(
            flops=2 * ring * chunks * CAP * count * half,
            bytes_accessed=2 * ring * chunks * MAIN * width,
            transcendentals=0,
        ),
        name="early_dispatch",
    )(pair, ids_t, tokens)


def ffn_kernel(*refs):
    late_in, early_in, gate_w, up_w, down_w, late_made, early_made, in_sems, out_sems = refs[-9:]
    places, chunks, _, width = late_in.shape
    late_hbm, late_out, early_out = refs[:places], refs[places + 4 : -10], refs[-10]
    early_hbm, gate_hbm, up_hbm, down_hbm = refs[places : places + 4]
    model = gate_w.shape[1]
    half = model // 2
    main = chunks * MAIN
    last = 2 * chunks
    first, second = pl.ds(0, half), pl.ds(half, half)
    body, tail = pl.ds(0, half), pl.ds(half, width - half)

    reads = {}

    def read(name, source, target):
        reads[name] = pltpu.make_async_copy(source, target, in_sems.at[len(reads)])
        reads[name].start()

    def read_rows(j):
        read(("late", j), late_hbm[j], late_in.at[j])
        read(("early", j), early_hbm.at[:, j], early_in.at[j])

    read("gate_first", gate_hbm.at[0, :, first], gate_w.at[:, first])
    read(("late", 0), late_hbm[0], late_in.at[0])
    read("up_first", up_hbm.at[0, :, first], up_w.at[:, first])
    read(("early", 0), early_hbm.at[:, 0], early_in.at[0])
    read("gate_second", gate_hbm.at[0, :, second], gate_w.at[:, second])
    read("up_second", up_hbm.at[0, :, second], up_w.at[:, second])
    read("down", down_hbm.at[0], down_w)
    for j in range(1, places):
        read_rows(j)

    waited = set()

    def ready(*names):
        for name in names:
            if name not in waited:
                waited.add(name)
                reads[name].wait()

    writes = []

    def write(source, target):
        writes.append(pltpu.make_async_copy(source, target, out_sems.at[len(writes)]))
        writes[-1].start()

    def half_expert(late, early, j=None):
        if j is not None:
            ready("gate_first", ("late", j))
        gate = exact_dot(late(), gate_w[:, :half], ((1,), (1,)))
        ready("up_first")
        up = exact_dot(late(), up_w[:, :half], ((1,), (1,)))
        if j is not None:
            ready(("early", j), "gate_second")
        gate = gate + exact_dot(early(), gate_w[:, half:], ((1,), (1,)))
        ready("up_second")
        up = up + exact_dot(early(), up_w[:, half:], ((1,), (1,)))
        hidden = (gate / (1.0 + jnp.exp(-gate)) * up).astype(jnp.bfloat16)
        ready("down")
        late_value = exact_dot(hidden, down_w[:, :half]).astype(jnp.bfloat16)
        early_value = exact_dot(hidden, down_w[:, half:]).astype(jnp.bfloat16)
        return late_value, early_value

    for j in range(places):
        late_value, early_value = half_expert(
            lambda: late_in[j, :, :, :half].reshape(main, half),
            lambda: early_in[j, :, :, :half].reshape(main, half),
            j,
        )
        late_made[j, :, :, :half] = late_value.reshape(chunks, MAIN, half)
        write(late_made.at[j, :, :, body], late_out[j].at[:, :, body])
        early_made[j, :, :, :half] = early_value.reshape(chunks, MAIN, half)
        write(early_made.at[j, :, :, body], early_out.at[:, j, :, body])

    matrix = split_matrix()

    def gather_last(buffer):
        return pieces_to_rows(buffer[:, :, :, half:].reshape(places * main, width - half), matrix)

    late_rows, early_rows = gather_last(late_in), gather_last(early_in)
    late_value, early_value = half_expert(lambda: late_rows, lambda: early_rows)
    for value, made in ((late_value, late_made), (early_value, early_made)):
        for j in range(places):
            pieces = rows_to_pieces(value[last * j : last * (j + 1)], matrix)
            made[j, :, :, half:] = pieces.reshape(chunks, MAIN, width - half)
    for j in range(places):
        write(late_made.at[j, :, :, tail], late_out[j].at[:, :, tail])
        write(early_made.at[j, :, :, tail], early_out.at[:, j, :, tail])
    for copy in writes:
        copy.wait()


def half_ffn(late, early, w_gate, w_up, w_down):
    places = len(late)
    chunks, _, width = late[0].shape
    model, hidden = w_gate.shape[1:]
    rows = places * chunks * CAP
    outside = pl.BlockSpec(memory_space=pltpu.HBM)
    buffer = pltpu.VMEM((places, chunks, MAIN, width), jnp.bfloat16)
    late_shape = jax.ShapeDtypeStruct(late[0].shape, jnp.bfloat16)
    *late_out, early_out = pl.pallas_call(
        ffn_kernel,
        in_specs=[outside] * (places + 4),
        out_specs=[outside] * (places + 1),
        out_shape=[late_shape] * places + [jax.ShapeDtypeStruct(early.shape, jnp.bfloat16)],
        scratch_shapes=[
            buffer,
            buffer,
            pltpu.VMEM((hidden, model), jnp.bfloat16),
            pltpu.VMEM((hidden, model), jnp.bfloat16),
            pltpu.VMEM((hidden, model), jnp.bfloat16),
            buffer,
            buffer,
            pltpu.SemaphoreType.DMA((2 * places + 5,)),
            pltpu.SemaphoreType.DMA((4 * places,)),
        ],
        cost_estimate=pl.CostEstimate(
            flops=6 * rows * model * hidden,
            bytes_accessed=4 * rows * model + 6 * model * hidden,
            transcendentals=rows * hidden,
        ),
        compiler_params=pltpu.CompilerParams(vmem_limit_bytes=62 * 1024 * 1024),
        name="half_ffn",
    )(*late, early, w_gate.swapaxes(1, 2), w_up.swapaxes(1, 2), w_down)
    return late_out, early_out


def sum_halves_kernel(a_ref, b_ref, c_ref, d_ref, out_ref):
    for r, (first, second) in enumerate(((a_ref, b_ref), (c_ref, d_ref))):
        for i in range(0, first.shape[0], 8):
            both = first[i : i + 8].astype(jnp.float32) + second[i : i + 8].astype(jnp.float32)
            out_ref[i : i + 8, r] = both.astype(jnp.bfloat16)


def sum_halves(arrays):
    chunks, _, width = arrays[0].shape
    on_chip = pl.BlockSpec(memory_space=pltpu.VMEM)
    return pl.pallas_call(
        sum_halves_kernel,
        in_specs=[on_chip] * RING,
        out_specs=on_chip,
        out_shape=jax.ShapeDtypeStruct((chunks, 2, MAIN, width), jnp.bfloat16),
        cost_estimate=pl.CostEstimate(
            flops=4 * chunks * MAIN * width, bytes_accessed=12 * chunks * MAIN * width,
            transcendentals=0,
        ),
        compiler_params=pltpu.CompilerParams(vmem_limit_bytes=12 * 1024 * 1024),
        name="sum_halves",
    )(*arrays)


def early_combine_kernel(pair_ref, ids_ref, gates_ref, rows_ref, out_ref):
    chunks = rows_ref.shape[0]
    _, count, half = out_ref.shape
    expert = own_pair(chunks, count, pair_ref[0])
    slot, weight = slots_of(ids_ref[0], expert, gates_ref[0])
    main = rows_ref[:, 0, :, :half].reshape(chunks * MAIN, half)
    pieces = rows_ref[:, 0, :, half:].reshape(chunks * MAIN, half // PIECES)
    out_ref[0] = combine_rows(slot, weight, main, pieces).astype(jnp.bfloat16)


def early_combine(pair, ids_t, gates_t, rows):
    chunks, ring, _, width = rows.shape
    count = ids_t.shape[2]
    half = width * MAIN // CAP
    return pl.pallas_call(
        early_combine_kernel,
        grid=(ring,),
        in_specs=[
            pl.BlockSpec(memory_space=pltpu.SMEM),
            pl.BlockSpec((1,) + ids_t.shape[1:], lambda i: (i, 0, 0)),
            pl.BlockSpec((1,) + gates_t.shape[1:], lambda i: (i, 0, 0)),
            pl.BlockSpec((chunks, 1, MAIN, width), lambda i: (0, i, 0, 0)),
        ],
        out_specs=pl.BlockSpec((1, count, half), lambda i: (i, 0, 0)),
        out_shape=jax.ShapeDtypeStruct((ring, count, half), jnp.bfloat16),
        cost_estimate=pl.CostEstimate(
            flops=2 * ring * chunks * CAP * count * half,
            bytes_accessed=2 * ring * chunks * MAIN * width,
            transcendentals=0,
        ),
        name="early_combine",
    )(pair, ids_t, gates_t, rows)


def final_kernel(pair_ref, ids_ref, gates_ref, rows_ref, *refs):
    parts, (out_ref, slot_ref, weight_ref) = refs[:RING], refs[RING:]
    experts = rows_ref.shape[0]
    half = parts[0].shape[1]
    block = 16
    expert = near_first(*slot_ref.shape, pair_ref[0])
    slot, weight = slots_of(ids_ref[...], expert, gates_ref[...])
    slot_ref[...] = slot
    weight_ref[...] = weight
    total = jnp.zeros((slot.shape[1], half), jnp.float32)
    for first in range(0, experts, block):
        here = slice(first, first + block)
        main = rows_ref[here, :, :half].reshape(block * MAIN, half)
        pieces = rows_ref[here, :, half:].reshape(block * MAIN, half // PIECES)
        total += combine_rows(slot_ref[here, :], weight_ref[here, :], main, pieces)
    out_ref[:, :half] = total.astype(jnp.bfloat16)
    total = parts[0][...].astype(jnp.float32)
    for part in parts[1:]:
        total += part[...].astype(jnp.float32)
    out_ref[:, half:] = total.astype(jnp.bfloat16)


def final_combine(pair, ids_t, gates_t, rows, parts):
    experts, _, width = rows.shape
    count, half = parts[0].shape
    on_chip = pl.BlockSpec(memory_space=pltpu.VMEM)
    return pl.pallas_call(
        final_kernel,
        in_specs=[pl.BlockSpec(memory_space=pltpu.SMEM)] + [on_chip] * (3 + RING),
        out_specs=on_chip,
        out_shape=jax.ShapeDtypeStruct((count, 2 * half), jnp.bfloat16),
        scratch_shapes=[
            pltpu.VMEM((experts, count), jnp.float32),
            pltpu.VMEM((experts, count), jnp.float32),
        ],
        cost_estimate=pl.CostEstimate(
            flops=2 * experts * CAP * count * half,
            bytes_accessed=2 * experts * MAIN * width,
            transcendentals=0,
        ),
        compiler_params=pltpu.CompilerParams(vmem_limit_bytes=16 * 1024 * 1024),
        name="final_combine",
    )(pair, ids_t, gates_t, rows, *parts)


def across(array, j):
    return lax.ppermute(array, "y", [(y, y ^ j) for y in range(RING)])


def at_places(array):
    arrays = [array]
    for j in range(1, RING):
        arrays.append(across(array, j))
    return arrays


def plane_exchange(array):
    return lax.all_to_all(array, PLANE, split_axis=0, concat_axis=0, tiled=True)


def per_device(tokens, expert_ids, gate_weights, w_gate, w_up, w_down):
    chunks = lax.axis_size("grp") * lax.axis_size("x")
    experts = 2 * chunks
    top = expert_ids.shape[1]
    half = tokens.shape[1] // 2
    pair = (lax.axis_index("y") // 2).astype(jnp.int32).reshape(1)
    ids_t = expert_ids.T
    gates_t = gate_weights.T

    late = late_dispatch(pair, ids_t, tokens, experts)
    width = late.shape[2]
    late = plane_exchange(late.reshape(chunks, 2 * MAIN, width))
    late = late.reshape(chunks, 2, MAIN, width)
    near, far = late[:, 0], late[:, 1]

    routing = at_places(jnp.concatenate([ids_t.astype(jnp.bfloat16), gates_t], axis=0))
    tokens_at = at_places(tokens[:, half:])
    late_in = [near]
    for j in range(1, RING):
        late_in.append(across(near if j == 1 else far, j))
    late_back, parts = [None] * RING, [None] * RING
    arrived, ids_ring, gates_ring = [], [], []
    for batch, places in enumerate(BATCHES):
        table = jnp.stack([routing[j] for j in places])
        ids_ring.append(table[:, :top].astype(jnp.int32))
        gates_ring.append(table[:, top:].astype(jnp.float32))
        tokens_here = jnp.stack([tokens_at[j] for j in places])
        early = early_dispatch(pair, ids_ring[batch], tokens_here, chunks)
        early = plane_exchange(early.reshape(chunks, len(places) * MAIN, width))
        arrived.append(early.reshape(chunks, len(places), MAIN, width))

    early_back = []
    for batch, places in enumerate(BATCHES):
        late_out, early_out = half_ffn(
            [late_in[j] for j in places], arrived[batch], w_gate, w_up, w_down
        )
        for j, rows in zip(places, late_out):
            late_back[j] = across(rows, j) if j else rows
        early_back.append(plane_exchange(early_out.reshape(chunks, -1, width)))

    late_back = plane_exchange(sum_halves(late_back).reshape(chunks, 2 * MAIN, width))
    for batch, places in enumerate(BATCHES):
        rows = early_back[batch].reshape(chunks, len(places), MAIN, width)
        partial = early_combine(pair, ids_ring[batch], gates_ring[batch], rows)
        for i, j in enumerate(places):
            parts[j] = across(partial[i], j) if j else partial[i]
    return final_combine(
        pair, ids_t, gates_t.astype(jnp.float32), late_back.reshape(experts, MAIN, width), parts
    )


def solution(mesh):
    ring = Mesh(mesh.devices.reshape(mesh.devices.shape[0], -1, RING), AXES)
    rows = P(AXES, None)
    weights = P(AXES, None, None)

    return jax.shard_map(
        per_device,
        mesh=ring,
        in_specs=(rows, rows, rows, weights, weights, weights),
        out_specs=rows,
        check_vma=False,
    )
```

```python
import jax
import jax.numpy as jnp
from jax import lax
from jax.experimental import pallas as pl
from jax.experimental.pallas import tpu as pltpu
from jax.sharding import Mesh, PartitionSpec as P

AXES = ("grp", "x", "y")
PLANE = ("grp", "x")
CAP = 18
MAIN = 16
PIECES = 8
TILE = MAIN * PIECES
RING = 4
BATCHES = ((1, 3), (0, 2))


def split_matrix():
    row = lax.broadcasted_iota(jnp.int32, (TILE, TILE), 0)
    col = lax.broadcasted_iota(jnp.int32, (TILE, TILE), 1)
    source = (row % MAIN) // 2 * MAIN + (row % 2) * PIECES + row // MAIN
    return (source == col).astype(jnp.bfloat16)


def exact_dot(a, b, dims=((1,), (0,))):
    return lax.dot_general(a, b, (dims, ((), ())), preferred_element_type=jnp.float32)


def pieces_to_rows(pieces, matrix):
    tiles = []
    for tile in range(pieces.shape[0] // TILE):
        stacked = exact_dot(matrix, pieces[TILE * tile : TILE * (tile + 1)])
        stacked = stacked.astype(jnp.bfloat16)
        tiles.append(
            jnp.concatenate([stacked[MAIN * q : MAIN * (q + 1)] for q in range(PIECES)], axis=1)
        )
    return jnp.concatenate(tiles, axis=0)


def rows_to_pieces(rows, matrix):
    width = rows.shape[1] // PIECES
    tiles = []
    for tile in range(rows.shape[0] // MAIN):
        part = rows[MAIN * tile : MAIN * (tile + 1)]
        stacked = jnp.concatenate(
            [part[:, width * q : width * (q + 1)] for q in range(PIECES)], axis=0
        )
        tiles.append(exact_dot(matrix, stacked, ((0,), (0,))).astype(jnp.bfloat16))
    return jnp.concatenate(tiles, axis=0)


def slots_of(ids_t, expert, gates_t=None):
    count = ids_t.shape[1]
    used = jnp.zeros(expert.shape, jnp.float32)
    weight = jnp.zeros(expert.shape, jnp.float32)
    for k in range(ids_t.shape[0]):
        hit = expert == ids_t[k : k + 1, :]
        used = jnp.where(hit, 1.0, used)
        if gates_t is not None:
            weight = jnp.where(hit, gates_t[k : k + 1, :], weight)
    earlier = lax.broadcasted_iota(jnp.int32, (count, count), 0)
    later = lax.broadcasted_iota(jnp.int32, (count, count), 1)
    before = exact_dot(used.astype(jnp.bfloat16), (earlier < later).astype(jnp.bfloat16))
    return jnp.where(used > 0.0, before, -1.0), weight


def near_first(rows, count, pair):
    row = lax.broadcasted_iota(jnp.int32, (rows, count), 0)
    other = row % 2
    return row - other + jnp.where(other == 0, pair, 1 - pair)


def own_pair(rows, count, pair):
    return 2 * lax.broadcasted_iota(jnp.int32, (rows, count), 0) + pair


def pick_rows(slot, tokens):
    block, count = slot.shape
    model = tokens.shape[1]
    main_id = lax.broadcasted_iota(jnp.int32, (block, MAIN, count), 1).astype(jnp.float32)
    pick = (slot[:, None, :] == main_id).astype(jnp.float32).reshape(block * MAIN, count)
    rows = exact_dot(pick.astype(jnp.bfloat16), tokens).astype(jnp.bfloat16)
    row = lax.broadcasted_iota(jnp.int32, (2 * block, count), 0)
    slot_twice = jnp.broadcast_to(slot[:, None, :], (block, 2, count)).reshape(2 * block, count)
    pick_last = (slot_twice == (MAIN + row % 2).astype(jnp.float32)).astype(jnp.bfloat16)
    last = exact_dot(pick_last, tokens).astype(jnp.bfloat16)
    pieces = rows_to_pieces(last, split_matrix())
    return rows.reshape(block, MAIN, model), pieces.reshape(block, MAIN, model // PIECES)


def combine_rows(slot, weight, main, pieces):
    block, count = slot.shape

    def spread(first, slots):
        shape = (block, slots, count)
        slot_id = first + lax.broadcasted_iota(jnp.int32, shape, 1)
        hit = slot[:, None, :] == slot_id.astype(jnp.float32)
        scaled = jnp.where(hit, jnp.broadcast_to(weight[:, None, :], shape), 0.0)
        return scaled.reshape(block * slots, count).astype(jnp.bfloat16)

    total = exact_dot(spread(0, MAIN), main, ((0,), (0,)))
    last = pieces_to_rows(pieces, split_matrix())
    return total + exact_dot(spread(MAIN, CAP - MAIN), last, ((0,), (0,)))


def late_dispatch_kernel(pair_ref, ids_ref, tokens_ref, out_ref, slot_ref):
    block, _, _ = out_ref.shape
    model = tokens_ref.shape[1]
    step = pl.program_id(0)

    @pl.when(step == 0)
    def _():
        expert = near_first(*slot_ref.shape, pair_ref[0])
        slot_ref[...] = slots_of(ids_ref[...], expert)[0]

    slot = slot_ref[pl.ds(pl.multiple_of(step * block, block), block), :]
    rows, pieces = pick_rows(slot, tokens_ref[...])
    out_ref[:, :, :model] = rows
    out_ref[:, :, model:] = pieces


def late_dispatch(pair, ids_t, tokens, experts):
    count, model = tokens.shape
    half = model // 2
    width = half * CAP // MAIN
    block = 32
    return pl.pallas_call(
        late_dispatch_kernel,
        grid=(experts // block,),
        in_specs=[
            pl.BlockSpec(memory_space=pltpu.SMEM),
            pl.BlockSpec(ids_t.shape, lambda i: (0, 0)),
            pl.BlockSpec((count, half), lambda i: (0, 0)),
        ],
        out_specs=pl.BlockSpec((block, MAIN, width), lambda i: (i, 0, 0)),
        out_shape=jax.ShapeDtypeStruct((experts, MAIN, width), jnp.bfloat16),
        scratch_shapes=[pltpu.VMEM((experts, count), jnp.float32)],
        cost_estimate=pl.CostEstimate(
            flops=2 * experts * CAP * count * half,
            bytes_accessed=2 * experts * MAIN * width,
            transcendentals=0,
        ),
        name="late_dispatch",
    )(pair, ids_t, tokens)


def early_dispatch_kernel(pair_ref, ids_ref, tokens_ref, out_ref):
    chunks = out_ref.shape[0]
    _, count, model = tokens_ref.shape
    expert = own_pair(chunks, count, pair_ref[0])
    slot = slots_of(ids_ref[0], expert)[0]
    rows, pieces = pick_rows(slot, tokens_ref[0])
    out_ref[:, 0, :, :model] = rows
    out_ref[:, 0, :, model:] = pieces


def early_dispatch(pair, ids_t, tokens, chunks):
    ring, count, half = tokens.shape
    width = half * CAP // MAIN
    return pl.pallas_call(
        early_dispatch_kernel,
        grid=(ring,),
        in_specs=[
            pl.BlockSpec(memory_space=pltpu.SMEM),
            pl.BlockSpec((1,) + ids_t.shape[1:], lambda i: (i, 0, 0)),
            pl.BlockSpec((1, count, half), lambda i: (i, 0, 0)),
        ],
        out_specs=pl.BlockSpec((chunks, 1, MAIN, width), lambda i: (0, i, 0, 0)),
        out_shape=jax.ShapeDtypeStruct((chunks, ring, MAIN, width), jnp.bfloat16),
        cost_estimate=pl.CostEstimate(
            flops=2 * ring * chunks * CAP * count * half,
            bytes_accessed=2 * ring * chunks * MAIN * width,
            transcendentals=0,
        ),
        name="early_dispatch",
    )(pair, ids_t, tokens)


def ffn_kernel(*refs):
    late_in, early_in, gate_w, up_w, down_w, late_made, early_made, in_sems, out_sems = refs[-9:]
    places, chunks, _, width = late_in.shape
    late_hbm, late_out, early_out = refs[:places], refs[places + 4 : -10], refs[-10]
    early_hbm, gate_hbm, up_hbm, down_hbm = refs[places : places + 4]
    model = gate_w.shape[1]
    half = model // 2
    main = chunks * MAIN
    last = 2 * chunks
    first, second = pl.ds(0, half), pl.ds(half, half)
    body, tail = pl.ds(0, half), pl.ds(half, width - half)

    reads = {}

    def read(name, source, target):
        reads[name] = pltpu.make_async_copy(source, target, in_sems.at[len(reads)])
        reads[name].start()

    def read_rows(j):
        read(("late", j), late_hbm[j], late_in.at[j])
        read(("early", j), early_hbm.at[:, j], early_in.at[j])

    read("gate_first", gate_hbm.at[0, :, first], gate_w.at[:, first])
    read(("late", 0), late_hbm[0], late_in.at[0])
    read("up_first", up_hbm.at[0, :, first], up_w.at[:, first])
    read(("early", 0), early_hbm.at[:, 0], early_in.at[0])
    read("gate_second", gate_hbm.at[0, :, second], gate_w.at[:, second])
    read("up_second", up_hbm.at[0, :, second], up_w.at[:, second])
    read("down", down_hbm.at[0], down_w)
    for j in range(1, places):
        read_rows(j)

    waited = set()

    def ready(*names):
        for name in names:
            if name not in waited:
                waited.add(name)
                reads[name].wait()

    writes = []

    def write(source, target):
        writes.append(pltpu.make_async_copy(source, target, out_sems.at[len(writes)]))
        writes[-1].start()

    def half_expert(late, early, j=None):
        if j is not None:
            ready("gate_first", ("late", j))
        gate = exact_dot(late(), gate_w[:, :half], ((1,), (1,)))
        ready("up_first")
        up = exact_dot(late(), up_w[:, :half], ((1,), (1,)))
        if j is not None:
            ready(("early", j), "gate_second")
        gate = gate + exact_dot(early(), gate_w[:, half:], ((1,), (1,)))
        ready("up_second")
        up = up + exact_dot(early(), up_w[:, half:], ((1,), (1,)))
        hidden = (gate / (1.0 + jnp.exp(-gate)) * up).astype(jnp.bfloat16)
        ready("down")
        late_value = exact_dot(hidden, down_w[:, :half]).astype(jnp.bfloat16)
        early_value = exact_dot(hidden, down_w[:, half:]).astype(jnp.bfloat16)
        return late_value, early_value

    for j in range(places):
        late_value, early_value = half_expert(
            lambda: late_in[j, :, :, :half].reshape(main, half),
            lambda: early_in[j, :, :, :half].reshape(main, half),
            j,
        )
        late_made[j, :, :, :half] = late_value.reshape(chunks, MAIN, half)
        write(late_made.at[j, :, :, body], late_out[j].at[:, :, body])
        early_made[j, :, :, :half] = early_value.reshape(chunks, MAIN, half)
        write(early_made.at[j, :, :, body], early_out.at[:, j, :, body])

    matrix = split_matrix()

    def gather_last(buffer):
        return pieces_to_rows(buffer[:, :, :, half:].reshape(places * main, width - half), matrix)

    late_rows, early_rows = gather_last(late_in), gather_last(early_in)
    late_value, early_value = half_expert(lambda: late_rows, lambda: early_rows)
    for value, made in ((late_value, late_made), (early_value, early_made)):
        for j in range(places):
            pieces = rows_to_pieces(value[last * j : last * (j + 1)], matrix)
            made[j, :, :, half:] = pieces.reshape(chunks, MAIN, width - half)
    for j in range(places):
        write(late_made.at[j, :, :, tail], late_out[j].at[:, :, tail])
        write(early_made.at[j, :, :, tail], early_out.at[:, j, :, tail])
    for copy in writes:
        copy.wait()


def half_ffn(late, early, w_gate, w_up, w_down):
    places = len(late)
    chunks, _, width = late[0].shape
    model, hidden = w_gate.shape[1:]
    rows = places * chunks * CAP
    outside = pl.BlockSpec(memory_space=pltpu.HBM)
    buffer = pltpu.VMEM((places, chunks, MAIN, width), jnp.bfloat16)
    late_shape = jax.ShapeDtypeStruct(late[0].shape, jnp.bfloat16)
    *late_out, early_out = pl.pallas_call(
        ffn_kernel,
        in_specs=[outside] * (places + 4),
        out_specs=[outside] * (places + 1),
        out_shape=[late_shape] * places + [jax.ShapeDtypeStruct(early.shape, jnp.bfloat16)],
        scratch_shapes=[
            buffer,
            buffer,
            pltpu.VMEM((hidden, model), jnp.bfloat16),
            pltpu.VMEM((hidden, model), jnp.bfloat16),
            pltpu.VMEM((hidden, model), jnp.bfloat16),
            buffer,
            buffer,
            pltpu.SemaphoreType.DMA((2 * places + 5,)),
            pltpu.SemaphoreType.DMA((4 * places,)),
        ],
        cost_estimate=pl.CostEstimate(
            flops=6 * rows * model * hidden,
            bytes_accessed=4 * rows * model + 6 * model * hidden,
            transcendentals=rows * hidden,
        ),
        compiler_params=pltpu.CompilerParams(vmem_limit_bytes=62 * 1024 * 1024),
        name="half_ffn",
    )(*late, early, w_gate.swapaxes(1, 2), w_up.swapaxes(1, 2), w_down)
    return late_out, early_out


def sum_halves_kernel(a_ref, b_ref, c_ref, d_ref, out_ref):
    for r, (first, second) in enumerate(((a_ref, b_ref), (c_ref, d_ref))):
        for i in range(0, first.shape[0], 8):
            both = first[i : i + 8].astype(jnp.float32) + second[i : i + 8].astype(jnp.float32)
            out_ref[i : i + 8, r] = both.astype(jnp.bfloat16)


def sum_halves(arrays):
    chunks, _, width = arrays[0].shape
    on_chip = pl.BlockSpec(memory_space=pltpu.VMEM)
    return pl.pallas_call(
        sum_halves_kernel,
        in_specs=[on_chip] * RING,
        out_specs=on_chip,
        out_shape=jax.ShapeDtypeStruct((chunks, 2, MAIN, width), jnp.bfloat16),
        cost_estimate=pl.CostEstimate(
            flops=4 * chunks * MAIN * width, bytes_accessed=12 * chunks * MAIN * width,
            transcendentals=0,
        ),
        compiler_params=pltpu.CompilerParams(vmem_limit_bytes=12 * 1024 * 1024),
        name="sum_halves",
    )(*arrays)


def early_combine_kernel(pair_ref, ids_ref, gates_ref, rows_ref, out_ref):
    chunks = rows_ref.shape[0]
    _, count, half = out_ref.shape
    expert = own_pair(chunks, count, pair_ref[0])
    slot, weight = slots_of(ids_ref[0], expert, gates_ref[0])
    main = rows_ref[:, 0, :, :half].reshape(chunks * MAIN, half)
    pieces = rows_ref[:, 0, :, half:].reshape(chunks * MAIN, half // PIECES)
    out_ref[0] = combine_rows(slot, weight, main, pieces).astype(jnp.bfloat16)


def early_combine(pair, ids_t, gates_t, rows):
    chunks, ring, _, width = rows.shape
    count = ids_t.shape[2]
    half = width * MAIN // CAP
    return pl.pallas_call(
        early_combine_kernel,
        grid=(ring,),
        in_specs=[
            pl.BlockSpec(memory_space=pltpu.SMEM),
            pl.BlockSpec((1,) + ids_t.shape[1:], lambda i: (i, 0, 0)),
            pl.BlockSpec((1,) + gates_t.shape[1:], lambda i: (i, 0, 0)),
            pl.BlockSpec((chunks, 1, MAIN, width), lambda i: (0, i, 0, 0)),
        ],
        out_specs=pl.BlockSpec((1, count, half), lambda i: (i, 0, 0)),
        out_shape=jax.ShapeDtypeStruct((ring, count, half), jnp.bfloat16),
        cost_estimate=pl.CostEstimate(
            flops=2 * ring * chunks * CAP * count * half,
            bytes_accessed=2 * ring * chunks * MAIN * width,
            transcendentals=0,
        ),
        name="early_combine",
    )(pair, ids_t, gates_t, rows)


def final_kernel(pair_ref, ids_ref, gates_ref, rows_ref, *refs):
    parts, out_ref = refs[:RING], refs[RING]
    experts = rows_ref.shape[0]
    half = parts[0].shape[1]
    expert = near_first(experts, ids_ref.shape[1], pair_ref[0])
    slot, weight = slots_of(ids_ref[...], expert, gates_ref[...])
    main = rows_ref[:, :, :half].reshape(experts * MAIN, half)
    pieces = rows_ref[:, :, half:].reshape(experts * MAIN, half // PIECES)
    out_ref[:, :half] = combine_rows(slot, weight, main, pieces).astype(jnp.bfloat16)
    total = parts[0][...].astype(jnp.float32)
    for part in parts[1:]:
        total += part[...].astype(jnp.float32)
    out_ref[:, half:] = total.astype(jnp.bfloat16)


def final_combine(pair, ids_t, gates_t, rows, parts):
    experts, _, width = rows.shape
    count, half = parts[0].shape
    on_chip = pl.BlockSpec(memory_space=pltpu.VMEM)
    return pl.pallas_call(
        final_kernel,
        in_specs=[pl.BlockSpec(memory_space=pltpu.SMEM)] + [on_chip] * (3 + RING),
        out_specs=on_chip,
        out_shape=jax.ShapeDtypeStruct((count, 2 * half), jnp.bfloat16),
        cost_estimate=pl.CostEstimate(
            flops=2 * experts * CAP * count * half,
            bytes_accessed=2 * experts * MAIN * width,
            transcendentals=0,
        ),
        compiler_params=pltpu.CompilerParams(vmem_limit_bytes=16 * 1024 * 1024),
        name="final_combine",
    )(pair, ids_t, gates_t, rows, *parts)


def across(array, j):
    return lax.ppermute(array, "y", [(y, y ^ j) for y in range(RING)])


def at_places(array):
    arrays = [array]
    for j in range(1, RING):
        arrays.append(across(array, j))
    return arrays


def plane_exchange(array):
    return lax.all_to_all(array, PLANE, split_axis=0, concat_axis=0, tiled=True)


def per_device(tokens, expert_ids, gate_weights, w_gate, w_up, w_down):
    chunks = lax.axis_size("grp") * lax.axis_size("x")
    experts = 2 * chunks
    top = expert_ids.shape[1]
    half = tokens.shape[1] // 2
    pair = (lax.axis_index("y") >> 1).astype(jnp.int32).reshape(1)
    ids_t = expert_ids.T
    gates_t = gate_weights.T

    late = late_dispatch(pair, ids_t, tokens, experts)
    width = late.shape[2]
    late = plane_exchange(late.reshape(chunks, 2 * MAIN, width))
    late = late.reshape(chunks, 2, MAIN, width)
    near, far = late[:, 0], late[:, 1]

    routing = at_places(jnp.concatenate([ids_t.astype(jnp.bfloat16), gates_t], axis=0))
    tokens_at = at_places(tokens[:, half:])
    late_in = [near]
    for j in range(1, RING):
        late_in.append(across(near if j == 1 else far, j))
    late_back, parts = [None] * RING, [None] * RING
    arrived, ids_ring, gates_ring = [], [], []
    for batch, places in enumerate(BATCHES):
        table = jnp.stack([routing[j] for j in places])
        ids_ring.append(table[:, :top].astype(jnp.int32))
        gates_ring.append(table[:, top:].astype(jnp.float32))
        tokens_here = jnp.stack([tokens_at[j] for j in places])
        early = early_dispatch(pair, ids_ring[batch], tokens_here, chunks)
        early = plane_exchange(early.reshape(chunks, len(places) * MAIN, width))
        arrived.append(early.reshape(chunks, len(places), MAIN, width))

    early_back = []
    for batch, places in enumerate(BATCHES):
        late_out, early_out = half_ffn(
            [late_in[j] for j in places], arrived[batch], w_gate, w_up, w_down
        )
        for j, rows in zip(places, late_out):
            late_back[j] = across(rows, j) if j else rows
        early_back.append(plane_exchange(early_out.reshape(chunks, -1, width)))

    late_back = plane_exchange(sum_halves(late_back).reshape(chunks, 2 * MAIN, width))
    for batch, places in enumerate(BATCHES):
        rows = early_back[batch].reshape(chunks, len(places), MAIN, width)
        partial = early_combine(pair, ids_ring[batch], gates_ring[batch], rows)
        for i, j in enumerate(places):
            parts[j] = across(partial[i], j) if j else partial[i]
    return final_combine(
        pair, ids_t, gates_t.astype(jnp.float32), late_back.reshape(experts, MAIN, width), parts
    )


def solution(mesh):
    ring = Mesh(mesh.devices.reshape(mesh.devices.shape[0], -1, RING), AXES)
    rows = P(AXES, None)
    weights = P(AXES, None, None)

    return jax.shard_map(
        per_device,
        mesh=ring,
        in_specs=(rows, rows, rows, weights, weights, weights),
        out_specs=rows,
        check_vma=False,
    )
```
